8 devices in a mesh: dp: 2 (over z, y), tp: 4 (over x, core).
Axes of the slice: x: 2, y: 2, z: 1, core: 2. Of those that a mesh axis runs over, the one named last changes fastest.
Arguments:
- x: bfloat16 [64, 4096], P('dp'), parts along dimension 0
- k_cache: bfloat16 [64, 1024, 32, 128], P('dp', None, 'tp'), parts along dimension 0
- v_cache: bfloat16 [64, 1024, 32, 128], P('dp', None, 'tp'), parts along dimension 0
- seq_lens: int32 [64], P('dp'), parts along dimension 0
- nbr_enc: bfloat16 [64, 256, 896], P('dp', 'tp'), parts along dimension 0
- ln1_gain: float32 [4096], replicated
- ln1_bias: float32 [4096], replicated
- w_q: bfloat16 [4096, 4096], P(None, 'tp')
- w_k: bfloat16 [4096, 4096], P(None, 'tp')
- w_v: bfloat16 [4096, 4096], P(None, 'tp')
- w_o: bfloat16 [4096, 4096], P('tp')
- ln2_gain: float32 [4096], replicated
- ln2_bias: float32 [4096], replicated
- wq_c: bfloat16 [4096, 4096], P(None, 'tp')
- wk_c: bfloat16 [896, 4096], P(None, 'tp')
- wv_c: bfloat16 [896, 4096], P(None, 'tp')
- wo_c: bfloat16 [4096, 4096], P('tp')
- ln3_gain: float32 [4096], replicated
- ln3_bias: float32 [4096], replicated
- w_up: bfloat16 [4096, 16384], P(None, 'tp')
- w_down: bfloat16 [16384, 4096], P('tp')
Outputs:
- output 1: bfloat16 [64, 4096], P('dp'), parts along dimension 0
- output 2: bfloat16 [64, 32, 128], P('dp', 'tp'), parts along dimension 0
- output 3: bfloat16 [64, 32, 128], P('dp', 'tp'), parts along dimension 0
There are 2 independent parts. The reference program is written for one: setup_inputs(seed, part) draws one part's arguments, and reference() takes and returns one part's arrays. A program takes and returns all parts, laid end to end along the dimension named above; an argument that names none is the same for every part.
All inputs are finite; a program needn't handle non-finite values.
Results may differ from the reference program's by a relative error of at most 0.0149296.
Values are sent between devices in bfloat16 or wider.
A program may use at most 1 GiB of HBM per device.

```python
import jax
import jax.numpy as jnp
from jax import lax

D = 4096
HEADS = 32
HEAD = 128
ENC_DIM = 896
NEIGHBOURS = 2
RET_LEN = 128
SEGMENT = 64
BATCH = 32
CTX_LEN = 1024

FF_DIM = 4 * D
WIDTH = HEADS * HEAD
NBR_TOKENS = NEIGHBOURS * RET_LEN
LN_EPS = 1e-5


def draw_lens(key):
    key_len, key_pick = jax.random.split(key)
    top_seg = CTX_LEN // SEGMENT - 1
    seg_count = jax.random.randint(key_len, (BATCH,), 1, top_seg + 1)
    pick_row = jax.random.randint(key_pick, (), 0, BATCH)
    seg_count = jnp.where(jnp.arange(BATCH) == pick_row, top_seg, seg_count)
    return (seg_count * SEGMENT).astype(jnp.int32)


def draw_weight(key, fan_in, fan_out, gain):
    return (jax.random.normal(key, (fan_in, fan_out), jnp.float32) * (gain * fan_in ** -0.5)).astype(jnp.bfloat16)


def setup_inputs(seed: int = 0, part: int = 0) -> dict:
    own_keys = jax.random.split(jax.random.fold_in(jax.random.key(seed), part), 8)
    shared_keys = jax.random.split(jax.random.key(seed + 1), 12)
    ramp = (2.0 * jnp.arange(CTX_LEN, dtype=jnp.float32) / CTX_LEN - 1.0)[None, :, None, None]
    cache_shape = (BATCH, CTX_LEN, HEADS, HEAD)
    head_shape = (BATCH, 1, HEADS, HEAD)
    k_dir = jax.random.normal(own_keys[1], head_shape, jnp.float32)
    k_cache = 3.0 * ramp * k_dir + jax.random.normal(own_keys[2], cache_shape, jnp.float32)
    v_base = jax.random.normal(own_keys[3], head_shape, jnp.float32)
    v_dir = jax.random.normal(own_keys[4], head_shape, jnp.float32)
    v_cache = v_base + ramp * v_dir + 0.5 * jax.random.normal(own_keys[5], cache_shape, jnp.float32)
    nbr_enc = jax.random.normal(own_keys[7], (BATCH, NBR_TOKENS, ENC_DIM), jnp.float32)
    ln_gains = 1.0 + 0.4 * jax.random.normal(shared_keys[0], (3, D), jnp.float32)
    ln_biases = 0.4 * jax.random.normal(shared_keys[1], (3, D), jnp.float32)
    return {
        'x': jax.random.normal(own_keys[0], (BATCH, D), jnp.float32).astype(jnp.bfloat16),
        'k_cache': k_cache.astype(jnp.bfloat16),
        'v_cache': v_cache.astype(jnp.bfloat16),
        'seq_lens': draw_lens(own_keys[6]),
        'nbr_enc': nbr_enc.astype(jnp.bfloat16),
        'ln1_gain': ln_gains[0],
        'ln1_bias': ln_biases[0],
        'w_q': draw_weight(shared_keys[2], D, WIDTH, 1.0),
        'w_k': draw_weight(shared_keys[3], D, WIDTH, 1.0),
        'w_v': draw_weight(shared_keys[4], D, WIDTH, 1.0),
        'w_o': draw_weight(shared_keys[5], WIDTH, D, 1.0),
        'ln2_gain': ln_gains[1],
        'ln2_bias': ln_biases[1],
        'wq_c': draw_weight(shared_keys[6], D, WIDTH, 1.0),
        'wk_c': draw_weight(shared_keys[7], ENC_DIM, WIDTH, 2.5),
        'wv_c': draw_weight(shared_keys[8], ENC_DIM, WIDTH, 1.0),
        'wo_c': draw_weight(shared_keys[9], WIDTH, D, 1.0),
        'ln3_gain': ln_gains[2],
        'ln3_bias': ln_biases[2],
        'w_up': draw_weight(shared_keys[10], D, FF_DIM, 1.0),
        'w_down': draw_weight(shared_keys[11], FF_DIM, D, 1.5),
    }


def layer_norm(values, ln_gain, ln_bias):
    row_mean = jnp.mean(values, axis=-1, keepdims=True)
    centred = values - row_mean
    row_var = jnp.mean(jnp.square(centred), axis=-1, keepdims=True)
    return (centred * lax.rsqrt(row_var + LN_EPS) * ln_gain + ln_bias).astype(jnp.bfloat16)


def project(operand, weight):
    return jnp.dot(operand, weight, preferred_element_type=jnp.float32).astype(jnp.bfloat16)


def reference(x, k_cache, v_cache, seq_lens, nbr_enc, ln1_gain, ln1_bias, w_q, w_k, w_v, w_o, ln2_gain, ln2_bias, wq_c, wk_c, wv_c, wo_c, ln3_gain, ln3_bias, w_up, w_down):
    q_scale = HEAD ** -0.5
    positions = jnp.arange(CTX_LEN)
    residual = x.astype(jnp.float32)
    a_norm = layer_norm(residual, ln1_gain, ln1_bias)
    q_new = project(a_norm, w_q).reshape(BATCH, HEADS, HEAD)
    k_new = project(a_norm, w_k).reshape(BATCH, HEADS, HEAD)
    v_new = project(a_norm, w_v).reshape(BATCH, HEADS, HEAD)

    def self_row(row_args):
        q_row, k_rows, v_rows, k_one, v_one, length = row_args
        q_f = q_row.astype(jnp.float32)
        s_old = jnp.einsum('hd,thd->ht', q_f, k_rows.astype(jnp.float32)) * q_scale
        s_old = jnp.where(positions[None, :] < length, s_old, -1e30)
        s_new = jnp.sum(q_f * k_one.astype(jnp.float32), axis=-1) * q_scale
        row_max = jnp.maximum(jnp.max(s_old, axis=-1), s_new)
        e_old = jnp.exp(s_old - row_max[:, None])
        e_new = jnp.exp(s_new - row_max)
        row_sum = jnp.sum(e_old, axis=-1) + e_new
        p_old = (e_old / row_sum[:, None]).astype(jnp.bfloat16).astype(jnp.float32)
        p_new = (e_new / row_sum).astype(jnp.bfloat16).astype(jnp.float32)
        head_out = jnp.einsum('ht,thd->hd', p_old, v_rows.astype(jnp.float32)) + p_new[:, None] * v_one.astype(jnp.float32)
        return head_out.astype(jnp.bfloat16)

    def cross_row(row_args):
        q_row, enc_row = row_args
        k_nbr = project(enc_row, wk_c).reshape(NBR_TOKENS, HEADS, HEAD).astype(jnp.float32)
        v_nbr = project(enc_row, wv_c).reshape(NBR_TOKENS, HEADS, HEAD).astype(jnp.float32)
        scores = jnp.einsum('hd,nhd->hn', q_row.astype(jnp.float32), k_nbr) * q_scale
        probs = jax.nn.softmax(scores, axis=-1).astype(jnp.bfloat16).astype(jnp.float32)
        return jnp.einsum('hn,nhd->hd', probs, v_nbr).astype(jnp.bfloat16)

    self_out = lax.map(self_row, (q_new, k_cache, v_cache, k_new, v_new, seq_lens))
    residual = residual + project(self_out.reshape(BATCH, WIDTH), w_o).astype(jnp.float32)
    c_norm = layer_norm(residual, ln2_gain, ln2_bias)
    q_cross = project(c_norm, wq_c).reshape(BATCH, HEADS, HEAD)
    cross_out = lax.map(cross_row, (q_cross, nbr_enc))
    residual = residual + project(cross_out.reshape(BATCH, WIDTH), wo_c).astype(jnp.float32)
    m_norm = layer_norm(residual, ln3_gain, ln3_bias)
    hidden = jax.nn.gelu(jnp.dot(m_norm, w_up, preferred_element_type=jnp.float32), approximate=False).astype(jnp.bfloat16)
    layer_out = (residual + project(hidden, w_down).astype(jnp.float32)).astype(jnp.bfloat16)
    return layer_out, k_new, v_new
```

```python
import jax
import jax.numpy as jnp
from jax import lax
from jax.experimental import pallas as pl
from jax.experimental.pallas import tpu as pltpu
from jax.sharding import PartitionSpec as P

LN_EPS = 1e-5
LOG2_E = 1.4426950408889634
W_SLOTS = 8
W_ROWS = 512
SPAN = 64
GROUP = 8
KV_SLOTS = 5


def attn_kernel(lens_ref, x_ref, g_ref, b_ref, wq_ref, wk_ref, wv_ref, kc_ref, vc_ref,
                o_ref, kn_ref, vn_ref,
                w_buf, k_buf, v_buf, a_scr, q_scr, qb_scr, k_scr, v_scr, s_scr, o_scr, acc_scr, item_row, item_src, item_pos, w_sem, k_sem, v_sem):
    batch, width = x_ref.shape
    heads = q_scr.shape[1]
    head_dim = q_scr.shape[2]
    rate = head_dim ** -0.5 * LOG2_E
    w_chunks = width // W_ROWS
    span_rows = SPAN * heads
    half = span_rows // 2
    weights = (wq_ref, wk_ref, wv_ref)

    def w_copy(index, src, row):
        slot = lax.rem(index, W_SLOTS)
        return pltpu.make_async_copy(src.at[pl.ds(row * W_ROWS, W_ROWS), :], w_buf.at[slot], w_sem.at[slot])

    for index in range(W_SLOTS):
        w_copy(jnp.int32(index), weights[index // w_chunks], index % w_chunks).start()

    def list_row(row, count):
        def list_span(span, count):
            item_row[count] = row
            item_src[count] = row
            item_pos[count] = span * span_rows
            return count + 1
        return lax.fori_loop(0, lax.div(lens_ref[row], SPAN), list_span, count)
    items = lax.fori_loop(0, batch, list_row, jnp.int32(0))
    groups = lax.div(items + (GROUP - 1), GROUP)
    for extra in range(GROUP):
        item_row[items + extra] = batch
        item_src[items + extra] = 0
        item_pos[items + extra] = 0

    def kv_start(group):
        slot = lax.rem(group, KV_SLOTS)
        for member in range(GROUP):
            item = group * GROUP + member
            rows = pl.ds(pl.multiple_of(item_pos[item], span_rows), span_rows)
            place = pl.ds(member * span_rows, span_rows)
            pltpu.make_async_copy(kc_ref.at[item_src[item], rows], k_buf.at[slot, place], k_sem.at[slot]).start()
            pltpu.make_async_copy(vc_ref.at[item_src[item], rows], v_buf.at[slot, place], v_sem.at[slot]).start()

    values = x_ref[...].astype(jnp.float32)
    row_mean = jnp.mean(values, axis=-1, keepdims=True)
    centred = values - row_mean
    row_var = jnp.mean(jnp.square(centred), axis=-1, keepdims=True)
    normed = (centred * lax.rsqrt(row_var + LN_EPS) * g_ref[...] + b_ref[...]).astype(jnp.bfloat16)
    for chunk in range(w_chunks):
        a_scr[chunk] = normed[:, chunk * W_ROWS:(chunk + 1) * W_ROWS]

    acc_scr[...] = jnp.zeros_like(acc_scr)

    def step(index, carry):
        which = lax.div(index, w_chunks)
        chunk = lax.rem(index, w_chunks)
        slot = lax.rem(index, W_SLOTS)
        w_copy(index, wq_ref, chunk).wait()
        acc_scr[which] += jnp.dot(a_scr[chunk], w_buf[slot], preferred_element_type=jnp.float32)
        later = index + W_SLOTS
        for source in range(1, 3):
            @pl.when(lax.div(later, w_chunks) == source)
            def _():
                w_copy(later, weights[source], lax.rem(later, w_chunks)).start()

        for ahead in range(KV_SLOTS - 1):
            @pl.when((index == 2 * w_chunks + ahead) & (ahead < groups))
            def _():
                kv_start(jnp.int32(ahead))
        return carry
    lax.fori_loop(0, 3 * w_chunks, step, 0)

    for which in range(3):
        out = acc_scr[which].astype(jnp.bfloat16)
        if which == 1:
            kn_ref[...] = out
        if which == 2:
            vn_ref[...] = out
        rounded = out.astype(jnp.float32)
        dest = (q_scr, k_scr, v_scr)[which]
        for head in range(heads):
            dest[0:batch, head, :] = rounded[:, head * head_dim:(head + 1) * head_dim]

    def prepare(row, carry):
        q = q_scr[row]
        zero = jnp.zeros_like(q)
        qb_scr[row] = jnp.concatenate([jnp.concatenate([q, zero], axis=1), jnp.concatenate([zero, q], axis=1)], axis=0).astype(jnp.bfloat16)
        s_scr[row] = jnp.broadcast_to(jnp.sum(q * k_scr[row], axis=-1, keepdims=True), q.shape)
        return carry
    lax.fori_loop(0, batch, prepare, 0, unroll=4)
    qb_scr[batch] = jnp.zeros(qb_scr.shape[1:], qb_scr.dtype)
    s_scr[batch] = jnp.zeros(s_scr.shape[1:], s_scr.dtype)
    v_scr[batch] = jnp.zeros(v_scr.shape[1:], v_scr.dtype)

    sub = lax.broadcasted_iota(jnp.int32, (2 * heads, half), 0)
    lane = lax.broadcasted_iota(jnp.int32, (2 * heads, half), 1)
    keep = ((lane ^ sub) & (heads - 1)) == 0

    def group_step(group, carry):
        run_max, run_sum, run_out = carry
        slot = lax.rem(group, KV_SLOTS)
        whole = pl.ds(0, GROUP * span_rows)

        @pl.when(group + KV_SLOTS - 1 < groups)
        def _():
            kv_start(group + KV_SLOTS - 1)
        pltpu.make_async_copy(kc_ref.at[0, whole], k_buf.at[slot], k_sem.at[slot]).wait()
        pltpu.make_async_copy(vc_ref.at[0, whole], v_buf.at[slot], v_sem.at[slot]).wait()
        rows = [item_row[group * GROUP + member] for member in range(GROUP)]
        scores = []
        for member in range(GROUP):
            base = member * span_rows
            k_cat = jnp.concatenate([k_buf[slot, base:base + half, :], k_buf[slot, base + half:base + 2 * half, :]], axis=1)
            s = lax.dot_general(qb_scr[rows[member]], k_cat, (((1,), (1,)), ((), ())), preferred_element_type=jnp.float32)
            scores.append(jnp.where(keep, s, -1e30))
        tops = []
        for s in scores:
            folded = jnp.maximum(s[:heads], s[heads:])
            tops.append(jnp.max(folded, axis=-1, keepdims=True))
        weights_in = [jnp.exp2((s - jnp.concatenate([top, top], axis=0)) * rate) for s, top in zip(scores, tops)]
        outs = []
        sums = []
        for member in range(GROUP):
            base = member * span_rows
            e = weights_in[member]
            sums.append(jnp.sum(e[:heads] + e[heads:], axis=-1, keepdims=True))
            v_cat = jnp.concatenate([v_buf[slot, base:base + half, :], v_buf[slot, base + half:base + 2 * half, :]], axis=1)
            both = jnp.dot(e.astype(jnp.bfloat16), v_cat, preferred_element_type=jnp.float32)
            outs.append(both[:heads, :head_dim] + both[heads:, head_dim:])
        for member in range(GROUP):
            row = rows[member]
            first = item_pos[group * GROUP + member] == 0
            run_max = jnp.where(first, s_scr[row], run_max)
            run_sum = jnp.where(first, 1.0, run_sum)
            run_out = jnp.where(first, v_scr[row], run_out)
            top = jnp.broadcast_to(tops[member], run_max.shape)
            new_max = jnp.maximum(run_max, top)
            keep_old = jnp.exp2((run_max - new_max) * rate)
            take_new = jnp.exp2((top - new_max) * rate)
            run_sum = run_sum * keep_old + take_new * sums[member]
            run_out = run_out * keep_old + take_new * outs[member]
            run_max = new_max
            o_scr[row] = run_out / run_sum
        return run_max, run_sum, run_out
    blank = jnp.zeros((heads, head_dim), jnp.float32)
    lax.fori_loop(0, groups, group_step, (blank, blank, blank))
    for head in range(heads):
        o_ref[:, head * head_dim:(head + 1) * head_dim] = o_scr[0:batch, head, :].astype(jnp.bfloat16)


def self_block(x, k_cache, v_cache, seq_lens, gain, bias, w_q, w_k, w_v):
    batch, width = x.shape
    ctx, heads, head_dim = k_cache.shape[1:]
    k_flat = k_cache.reshape(batch, ctx * heads, head_dim)
    v_flat = v_cache.reshape(batch, ctx * heads, head_dim)
    vmem = pl.BlockSpec(memory_space=pltpu.VMEM)
    hbm = pl.BlockSpec(memory_space=pl.ANY)
    flat = jax.ShapeDtypeStruct((batch, heads * head_dim), jnp.bfloat16)
    per_head = pltpu.VMEM((batch + 1, heads, head_dim), jnp.float32)
    kv_buf = pltpu.VMEM((KV_SLOTS, GROUP * SPAN * heads, head_dim), jnp.bfloat16)
    most_items = batch * ctx // SPAN + GROUP
    return pl.pallas_call(
        attn_kernel,
        out_shape=(flat, flat, flat),
        in_specs=[pl.BlockSpec(memory_space=pltpu.SMEM), vmem, vmem, vmem, hbm, hbm, hbm, hbm, hbm],
        out_specs=(vmem, vmem, vmem),
        scratch_shapes=[
            pltpu.VMEM((W_SLOTS, W_ROWS, heads * head_dim), jnp.bfloat16),
            kv_buf, kv_buf,
            pltpu.VMEM((width // W_ROWS, batch, W_ROWS), jnp.bfloat16),
            per_head,
            pltpu.VMEM((batch + 1, 2 * heads, 2 * head_dim), jnp.bfloat16),
            per_head, per_head, per_head, per_head,
            pltpu.VMEM((3, batch, heads * head_dim), jnp.float32),
            pltpu.SMEM((most_items,), jnp.int32),
            pltpu.SMEM((most_items,), jnp.int32),
            pltpu.SMEM((most_items,), jnp.int32),
            pltpu.SemaphoreType.DMA((W_SLOTS,)),
            pltpu.SemaphoreType.DMA((KV_SLOTS,)),
            pltpu.SemaphoreType.DMA((KV_SLOTS,)),
        ],
        compiler_params=pltpu.CompilerParams(vmem_limit_bytes=60 * 1024 * 1024),
        name='self_block',
    )(seq_lens, x, gain.reshape(1, width), bias.reshape(1, width), w_q, w_k, w_v, k_flat, v_flat)


RING = 15
CUT = 256
QUAD = 512
SIDE = 1024


def mix_kernel(x_ref, o_ref, g2_ref, b2_ref, g3_ref, b3_ref, enc_ref, wo_ref, wq_ref, wk_ref, wv_ref, woc_ref, wup_ref, wdn_ref,
               out_ref,
               ring, e_buf, w_all, v_own, lhs, acc, h_scr, q_scr, q_send, q_recv, d_scr, p_scr, st_send, st_recv, o_mine, o_send, o_recv,
               ar_part, ar_half, ar_r1, ar_r2, ar_tot,
               ring_sem, e_sem, w_sem, ex_send, ex_recv, x_send, x_recv, y_send, y_recv, ar_send, ar_recv):
    batch, width = x_ref.shape
    head_dim = 128
    rate = head_dim ** -0.5 * LOG2_E
    dp = lax.axis_index('dp')
    tp = lax.axis_index('tp')
    core = lax.rem(tp, 2)
    mate = tp + 1 - 2 * core
    across = lax.rem(tp + 2, 4)
    other = 1 - dp
    to_mate, to_across, to_other = {'tp': mate}, {'tp': across}, {'dp': other}
    mesh_id = pl.DeviceIdType.MESH
    tokens = enc_ref.shape[1]
    spans = batch // 4

    barrier = pltpu.get_barrier_semaphore()
    for peer in (to_mate, to_across, to_other):
        pl.semaphore_signal(barrier, inc=1, device_id=peer, device_id_type=mesh_id)

    segments = ((wo_ref, 0, 4, False), (wq_ref, 4, 8, True), (woc_ref, 8, 12, False), (wup_ref, 12, 28, False), (wdn_ref, 28, 44, False))

    def ring_copy(src, deep, row, slot, piece):
        if deep:
            view = src.at[pl.ds(row * SIDE + piece * CUT, CUT), :]
        else:
            view = src.at[pl.ds(row * CUT, CUT), pl.ds(piece * SIDE, SIDE)]
        return pltpu.make_async_copy(view, ring.at[slot, piece], ring_sem.at[slot, piece])

    def ring_start(index):
        for src, low, high, deep in segments:
            @pl.when((index >= low) & (index < high))
            def _():
                for piece in range(4):
                    ring_copy(src, deep, index - low, lax.rem(index, RING), piece).start()

    def ring_wait(index):
        slot = lax.rem(index, RING)
        for piece in range(4):
            ring_copy(wo_ref, False, 0, slot, piece).wait()
        return slot

    def stream_wide(base, count):
        acc[...] = jnp.zeros_like(acc)

        def step(chunk, carry):
            slot = ring_wait(base + chunk)
            for piece in range(4):
                acc[piece] += jnp.dot(lhs[chunk], ring[slot, piece], preferred_element_type=jnp.float32)
            ring_start(base + chunk + RING)
            return carry
        lax.fori_loop(0, count, step, 0)

    for index in range(4):
        for piece in range(4):
            ring_copy(wo_ref, False, index, index, piece).start()
    mine = pl.ds(pl.multiple_of(core * tokens, tokens), tokens)
    e_local = pltpu.make_async_copy(enc_ref, e_buf.at[:, mine, :], e_sem)
    e_local.start()
    own_copies = []
    for kind, src in ((1, wv_ref), (0, wk_ref)):
        for quad in range(2):
            copy = pltpu.make_async_copy(src.at[:, pl.ds(quad * QUAD, QUAD)], w_all.at[kind, 0, quad], w_sem.at[kind, quad])
            copy.start()
            own_copies.append(copy)
    pl.semaphore_wait(barrier, 3)
    e_remote = pltpu.make_async_remote_copy(src_ref=enc_ref, dst_ref=e_buf.at[:, mine, :], send_sem=ex_send.at[0], recv_sem=ex_recv.at[0], device_id=to_mate, device_id_type=mesh_id)
    e_remote.start()

    def x_copy(unit):
        kind, column = unit // 4, unit % 4 * head_dim
        src = (wk_ref, wv_ref)[kind]
        start = pl.multiple_of(dp * QUAD + column, head_dim)
        return pltpu.make_async_remote_copy(src_ref=src.at[:, pl.ds(start, head_dim)], dst_ref=w_all.at[kind, 1, dp, :, pl.ds(column, head_dim)],
                                            send_sem=x_send.at[unit], recv_sem=x_recv.at[unit], device_id=to_across, device_id_type=mesh_id)

    def y_copy(unit):
        kind, column = unit // 4, unit % 4 * head_dim
        view = w_all.at[kind, 1, dp, :, pl.ds(column, head_dim)]
        return pltpu.make_async_remote_copy(src_ref=view, dst_ref=view, send_sem=y_send.at[unit], recv_sem=y_recv.at[unit], device_id=to_other, device_id_type=mesh_id)

    def relay(unit):
        x_copy(unit).wait_recv()
        y_copy(unit).start()

    for unit in range(8):
        x_copy(unit).start()
    for index in range(4, RING):
        ring_start(jnp.int32(index))

    def ar_copy(which, stage):
        if stage == 0:
            return pltpu.make_async_remote_copy(src_ref=ar_part.at[1 - core], dst_ref=ar_r1.at[which], send_sem=ar_send.at[which, 0], recv_sem=ar_recv.at[which, 0], device_id=to_mate, device_id_type=mesh_id)
        if stage == 1:
            return pltpu.make_async_remote_copy(src_ref=ar_half, dst_ref=ar_r2.at[which], send_sem=ar_send.at[which, 1], recv_sem=ar_recv.at[which, 1], device_id=to_across, device_id_type=mesh_id)
        return pltpu.make_async_remote_copy(src_ref=ar_tot.at[which, core], dst_ref=ar_tot.at[which, core], send_sem=ar_send.at[which, 2], recv_sem=ar_recv.at[which, 2], device_id=to_mate, device_id_type=mesh_id)

    def reduce_open(which):
        for half in range(2):
            for piece in range(2):
                ar_part[half, :, piece * SIDE:(piece + 1) * SIDE] = acc[half * 2 + piece].astype(jnp.bfloat16)
        ar_copy(which, 0).start()
        ar_copy(which, 0).wait()
        ar_half[...] = (ar_part[core].astype(jnp.float32) + ar_r1[which].astype(jnp.float32)).astype(jnp.bfloat16)
        ar_copy(which, 1).start()

    def reduce_close(which):
        ar_copy(which, 1).wait()
        ar_tot[which, core] = (ar_half[...].astype(jnp.float32) + ar_r2[which].astype(jnp.float32)).astype(jnp.bfloat16)
        ar_copy(which, 2).start()
        ar_copy(which, 2).wait()

    def total(which):
        return jnp.concatenate([ar_tot[which, 0].astype(jnp.float32), ar_tot[which, 1].astype(jnp.float32)], axis=1)

    def norm_into_lhs(values, gain_ref, bias_ref):
        row_mean = jnp.mean(values, axis=-1, keepdims=True)
        centred = values - row_mean
        row_var = jnp.mean(jnp.square(centred), axis=-1, keepdims=True)
        normed = (centred * lax.rsqrt(row_var + LN_EPS) * gain_ref[...] + bias_ref[...]).astype(jnp.bfloat16)
        for chunk in range(width // CUT):
            lhs[chunk] = normed[:, chunk * CUT:(chunk + 1) * CUT]

    def project_span(kind, side, quad, span):
        tile = e_buf[pl.ds(span * 4, 4)].reshape(4 * 2 * tokens, e_buf.shape[2])
        return jnp.dot(tile, w_all[kind, side, quad], preferred_element_type=jnp.float32).astype(jnp.bfloat16)

    row_id = lax.broadcasted_iota(jnp.int32, (16, QUAD), 0)
    col_tile = lax.broadcasted_iota(jnp.int32, (16, QUAD), 1) // head_dim
    head_match = row_id // 4 == col_tile
    seq_match = lax.rem(row_id, 4) == col_tile

    def keys_and_scores(side, quad):
        def step(span, carry):
            keys = project_span(0, side, quad, span)
            q4 = q_scr[side, quad, span]
            rows = jnp.where(head_match, jnp.concatenate([q4, q4, q4, q4], axis=0), 0.0).astype(jnp.bfloat16)
            s = lax.dot_general(rows, keys, (((1,), (1,)), ((), ())), preferred_element_type=jnp.float32)
            s = jnp.where(seq_match, s, 0.0)
            d_scr[side, quad, span] = s[:, 0:128] + s[:, 128:256] + s[:, 256:384] + s[:, 384:512]
            return carry
        lax.fori_loop(0, spans, step, 0, unroll=2)

    def own_values(quad):
        def step(span, carry):
            v_own[quad, span] = project_span(1, 0, quad, span)
            return carry
        lax.fori_loop(0, spans, step, 0, unroll=2)

    def apply_weights(side, quad, dest):
        def step(span, carry):
            values = v_own[quad, span] if side == 0 else project_span(1, side, quad, span)
            p = p_scr[side, quad, span]
            rows = jnp.where(seq_match, jnp.concatenate([p, p, p, p], axis=1), 0.0).astype(jnp.bfloat16)
            wide = jnp.dot(rows, values, preferred_element_type=jnp.float32)
            wide = jnp.where(head_match, wide, 0.0)
            dest[quad, span] = wide[0:4] + wide[4:8] + wide[8:12] + wide[12:16]
            return carry
        lax.fori_loop(0, spans, step, 0, unroll=2)

    for chunk in range(4):
        lhs[chunk] = o_ref[:, chunk * CUT:(chunk + 1) * CUT]
    stream_wide(0, 4)
    reduce_open(0)
    e_local.wait()
    e_remote.wait()
    own_copies[0].wait()
    own_values(0)
    relay(0)
    reduce_close(0)
    h_one = x_ref[...].astype(jnp.float32) + total(0)
    h_scr[...] = h_one
    norm_into_lhs(h_one, g2_ref, b2_ref)

    def query_step(chunk, carry):
        slot = ring_wait(4 + chunk)
        for piece in range(4):
            acc[0] += jnp.dot(lhs[chunk * 4 + piece], ring[slot, piece], preferred_element_type=jnp.float32)
        ring_start(4 + chunk + RING)
        return carry
    acc[0] = jnp.zeros_like(acc[0])
    lax.fori_loop(0, 4, query_step, 0)
    q_new = acc[0].astype(jnp.bfloat16)
    q_send[...] = q_new
    q_copy = pltpu.make_async_remote_copy(src_ref=q_send, dst_ref=q_recv, send_sem=ex_send.at[1], recv_sem=ex_recv.at[1], device_id=to_across, device_id_type=mesh_id)
    q_copy.start()
    relay(1)

    def spread_query(side, q):
        wide = q.astype(jnp.float32)
        for quad in range(2):
            for span in range(spans):
                q_scr[side, quad, span] = wide[span * 4:span * 4 + 4, quad * QUAD:(quad + 1) * QUAD]
    spread_query(0, q_new)
    own_copies[1].wait()
    own_values(1)
    relay(2)
    own_copies[2].wait()
    own_copies[3].wait()
    keys_and_scores(0, 0)
    relay(3)
    keys_and_scores(0, 1)
    relay(4)
    q_copy.wait()
    spread_query(1, q_recv[...])
    keys_and_scores(1, dp)
    relay(5)
    for unit in range(4):
        y_copy(unit).wait_recv()
    keys_and_scores(1, other)
    relay(6)

    lane = lax.broadcasted_iota(jnp.int32, (128, 128), 1)

    def block_stats(side, quad):
        s = d_scr[side, quad].reshape(128, 128)
        top = jnp.max(s, axis=-1, keepdims=True)
        part = jnp.sum(jnp.exp2((s - top) * rate), axis=-1, keepdims=True)
        return s, top, part

    for side in range(2):
        for quad in range(2):
            s, top, part = block_stats(side, quad)
            packed = jnp.where(lane == 0, top, jnp.where(lane == 1, part, 0.0))
            st_send[side, quad] = packed.T[0:8, :]
    st_copy = pltpu.make_async_remote_copy(src_ref=st_send, dst_ref=st_recv, send_sem=ex_send.at[2], recv_sem=ex_recv.at[2], device_id=to_across, device_id_type=mesh_id)
    st_copy.start()
    relay(7)
    st_copy.wait()
    for side in range(2):
        for quad in range(2):
            s, top, part = block_stats(side, quad)
            theirs = jnp.concatenate([st_recv[1 - side, quad], jnp.zeros((120, 128), jnp.float32)], axis=0).T
            their_top, their_part = theirs[:, 0:1], theirs[:, 1:2]
            whole_top = jnp.maximum(top, their_top)
            whole = part * jnp.exp2((top - whole_top) * rate) + their_part * jnp.exp2((their_top - whole_top) * rate)
            p = jnp.exp2((s - whole_top) * rate) / whole
            p_scr[side, quad] = p.reshape(8, 16, 128)
    apply_weights(0, 0, o_mine)
    apply_weights(0, 1, o_mine)

    def o_copy(slot, quad):
        return pltpu.make_async_remote_copy(src_ref=o_send.at[quad], dst_ref=o_recv.at[quad], send_sem=ex_send.at[3 + slot], recv_sem=ex_recv.at[3 + slot], device_id=to_across, device_id_type=mesh_id)
    apply_weights(1, dp, o_send)
    o_copy(0, dp).start()
    for unit in range(4, 8):
        y_copy(unit).wait_recv()
    apply_weights(1, other, o_send)
    o_copy(1, other).start()
    o_copy(0, dp).wait()
    o_copy(1, other).wait()
    for quad in range(2):
        whole = o_mine[quad] + o_recv[quad]
        whole = jnp.concatenate([whole[span] for span in range(spans)], axis=0).astype(jnp.bfloat16)
        for piece in range(2):
            lhs[quad * 2 + piece] = whole[:, piece * CUT:(piece + 1) * CUT]
    stream_wide(8, 4)
    reduce_open(1)
    reduce_close(1)
    h_two = h_scr[...] + total(1)
    h_scr[...] = h_two
    norm_into_lhs(h_two, g3_ref, b3_ref)
    stream_wide(12, 16)
    for piece in range(4):
        u = acc[piece]
        u = (0.5 * u * (1.0 + lax.erf(u * (0.5 ** 0.5)))).astype(jnp.bfloat16)
        for chunk in range(4):
            lhs[piece * 4 + chunk] = u[:, chunk * CUT:(chunk + 1) * CUT]
    stream_wide(28, 16)
    reduce_open(2)
    for unit in range(8):
        x_copy(unit).wait_send()
        y_copy(unit).wait_send()
    reduce_close(2)
    out_ref[...] = (h_scr[...] + total(2)).astype(jnp.bfloat16)


def mix_block(x, self_out, nbr_enc, ln2_gain, ln2_bias, wq_c, wk_c, wv_c, w_o, wo_c, ln3_gain, ln3_bias, w_up, w_down):
    batch, width = x.shape
    _, tokens, enc = nbr_enc.shape
    vmem = pl.BlockSpec(memory_space=pltpu.VMEM)
    hbm = pl.BlockSpec(memory_space=pl.ANY)
    spans = batch // 4
    bf, f32 = jnp.bfloat16, jnp.float32
    dma = pltpu.SemaphoreType.DMA
    half = width // 2
    return pl.pallas_call(
        mix_kernel,
        out_shape=jax.ShapeDtypeStruct((batch, width), bf),
        in_specs=[vmem] * 6 + [hbm] * 8,
        out_specs=vmem,
        scratch_shapes=[
            pltpu.VMEM((RING, 4, CUT, SIDE), bf),
            pltpu.VMEM((batch, 2 * tokens, enc), bf),
            pltpu.VMEM((2, 2, 2, enc, QUAD), bf),
            pltpu.VMEM((2, spans, 8 * tokens, QUAD), bf),
            pltpu.VMEM((width // CUT, batch, CUT), bf),
            pltpu.VMEM((4, batch, SIDE), f32),
            pltpu.VMEM((batch, width), f32),
            pltpu.VMEM((2, 2, spans, 4, QUAD), f32),
            pltpu.VMEM((batch, SIDE), bf),
            pltpu.VMEM((batch, SIDE), bf),
            pltpu.VMEM((2, 2, spans, 16, 128), f32),
            pltpu.VMEM((2, 2, spans, 16, 128), f32),
            pltpu.VMEM((2, 2, 8, 128), f32),
            pltpu.VMEM((2, 2, 8, 128), f32),
            pltpu.VMEM((2, spans, 4, QUAD), f32),
            pltpu.VMEM((2, spans, 4, QUAD), f32),
            pltpu.VMEM((2, spans, 4, QUAD), f32),
            pltpu.VMEM((2, batch, half), bf),
            pltpu.VMEM((batch, half), bf),
            pltpu.VMEM((3, batch, half), bf),
            pltpu.VMEM((3, batch, half), bf),
            pltpu.VMEM((3, 2, batch, half), bf),
            dma((RING, 4)), dma, dma((2, 2)), dma((5,)), dma((5,)), dma((8,)), dma((8,)), dma((8,)), dma((8,)), dma((3, 3)), dma((3, 3)),
        ],
        compiler_params=pltpu.CompilerParams(vmem_limit_bytes=67043328, collective_id=0, has_side_effects=True),
        name='mix_block',
    )(x, self_out, ln2_gain.reshape(1, width), ln2_bias.reshape(1, width), ln3_gain.reshape(1, width), ln3_bias.reshape(1, width), nbr_enc, w_o, wq_c, wk_c, wv_c, wo_c, w_up, w_down)


def local_step(x, k_cache, v_cache, seq_lens, nbr_enc, ln1_gain, ln1_bias, w_q, w_k, w_v, w_o, ln2_gain, ln2_bias, wq_c, wk_c, wv_c, wo_c, ln3_gain, ln3_bias, w_up, w_down):
    batch = x.shape[0]
    heads, head_dim = k_cache.shape[2:]
    self_out, k_new, v_new = self_block(x, k_cache, v_cache, seq_lens, ln1_gain, ln1_bias, w_q, w_k, w_v)
    layer_out = mix_block(x, self_out, nbr_enc, ln2_gain, ln2_bias, wq_c, wk_c, wv_c, w_o, wo_c, ln3_gain, ln3_bias, w_up, w_down)
    return layer_out, k_new.reshape(batch, heads, head_dim), v_new.reshape(batch, heads, head_dim)


def solution(mesh):
    row_spec = P('dp', None)
    cache_spec = P('dp', None, 'tp', None)
    head_spec = P('dp', 'tp', None)
    vec_spec = P(None)
    col_split = P(None, 'tp')
    row_split = P('tp', None)
    in_specs = (row_spec, cache_spec, cache_spec, P('dp'), P('dp', 'tp', None), vec_spec, vec_spec, col_split, col_split, col_split, row_split, vec_spec, vec_spec, col_split, col_split, col_split, row_split, vec_spec, vec_spec, col_split, row_split)
    out_specs = (row_spec, head_spec, head_spec)
    return jax.shard_map(local_step, mesh=mesh, in_specs=in_specs, out_specs=out_specs, check_vma=False)
```

```python
import jax
import jax.numpy as jnp
from jax import lax
from jax.experimental import pallas as pl
from jax.experimental.pallas import tpu as pltpu
from jax.sharding import PartitionSpec as P

LN_EPS = 1e-5
LOG2_E = 1.4426950408889634
W_SLOTS = 8
W_ROWS = 512
SPAN = 64
GROUP = 12
KV_SLOTS = 4


def attn_kernel(lens_ref, x_ref, g_ref, b_ref, wq_ref, wk_ref, wv_ref, kc_ref, vc_ref,
                o_ref, kn_ref, vn_ref,
                w_buf, k_buf, v_buf, a_scr, q_scr, qb_scr, k_scr, v_scr, s_scr, o_scr, acc_scr, item_row, item_src, item_pos, w_sem, k_sem, v_sem):
    batch, width = x_ref.shape
    heads = q_scr.shape[1]
    head_dim = q_scr.shape[2]
    rate = head_dim ** -0.5 * LOG2_E
    w_chunks = width // W_ROWS
    span_rows = SPAN * heads
    half = span_rows // 2
    weights = (wq_ref, wk_ref, wv_ref)

    def w_copy(index, src, row):
        slot = lax.rem(index, W_SLOTS)
        return pltpu.make_async_copy(src.at[pl.ds(row * W_ROWS, W_ROWS), :], w_buf.at[slot], w_sem.at[slot])

    for index in range(W_SLOTS):
        w_copy(jnp.int32(index), weights[index // w_chunks], index % w_chunks).start()

    def list_row(row, count):
        def list_span(span, count):
            item_row[count] = row
            item_src[count] = row
            item_pos[count] = span * span_rows
            return count + 1
        return lax.fori_loop(0, lax.div(lens_ref[row], SPAN), list_span, count)
    items = lax.fori_loop(0, batch, list_row, jnp.int32(0))
    groups = lax.div(items + (GROUP - 1), GROUP)
    for extra in range(GROUP):
        item_row[items + extra] = batch
        item_src[items + extra] = 0
        item_pos[items + extra] = 0

    def kv_start(group):
        slot = lax.rem(group, KV_SLOTS)
        for member in range(GROUP):
            item = group * GROUP + member
            rows = pl.ds(pl.multiple_of(item_pos[item], span_rows), span_rows)
            place = pl.ds(member * span_rows, span_rows)
            pltpu.make_async_copy(kc_ref.at[item_src[item], rows], k_buf.at[slot, place], k_sem.at[slot]).start()
            pltpu.make_async_copy(vc_ref.at[item_src[item], rows], v_buf.at[slot, place], v_sem.at[slot]).start()

    values = x_ref[...].astype(jnp.float32)
    row_mean = jnp.mean(values, axis=-1, keepdims=True)
    centred = values - row_mean
    row_var = jnp.mean(jnp.square(centred), axis=-1, keepdims=True)
    normed = (centred * lax.rsqrt(row_var + LN_EPS) * g_ref[...] + b_ref[...]).astype(jnp.bfloat16)
    for chunk in range(w_chunks):
        a_scr[chunk] = normed[:, chunk * W_ROWS:(chunk + 1) * W_ROWS]

    acc_scr[...] = jnp.zeros_like(acc_scr)

    def step(index, carry):
        which = lax.div(index, w_chunks)
        chunk = lax.rem(index, w_chunks)
        slot = lax.rem(index, W_SLOTS)
        w_copy(index, wq_ref, chunk).wait()
        acc_scr[which] += jnp.dot(a_scr[chunk], w_buf[slot], preferred_element_type=jnp.float32)
        later = index + W_SLOTS
        for source in range(1, 3):
            @pl.when(lax.div(later, w_chunks) == source)
            def _():
                w_copy(later, weights[source], lax.rem(later, w_chunks)).start()

        for ahead in range(KV_SLOTS - 1):
            @pl.when((index == 2 * w_chunks + ahead) & (ahead < groups))
            def _():
                kv_start(jnp.int32(ahead))
        return carry
    lax.fori_loop(0, 3 * w_chunks, step, 0)

    for which in range(3):
        out = acc_scr[which].astype(jnp.bfloat16)
        rounded = out.astype(jnp.float32)
        dest = (q_scr, k_scr, v_scr)[which]
        for head in range(heads):
            dest[0:batch, head, :] = rounded[:, head * head_dim:(head + 1) * head_dim]

    kn_ref[...] = k_scr[0:batch].astype(jnp.bfloat16)
    vn_ref[...] = v_scr[0:batch].astype(jnp.bfloat16)

    def prepare(row, carry):
        q = q_scr[row]
        zero = jnp.zeros_like(q)
        qb_scr[row] = jnp.concatenate([jnp.concatenate([q, zero], axis=1), jnp.concatenate([zero, q], axis=1)], axis=0).astype(jnp.bfloat16)
        s_scr[row] = jnp.broadcast_to(jnp.sum(q * k_scr[row], axis=-1, keepdims=True), q.shape)
        return carry
    lax.fori_loop(0, batch, prepare, 0, unroll=4)
    qb_scr[batch] = jnp.zeros(qb_scr.shape[1:], qb_scr.dtype)
    s_scr[batch] = jnp.zeros(s_scr.shape[1:], s_scr.dtype)
    v_scr[batch] = jnp.zeros(v_scr.shape[1:], v_scr.dtype)

    sub = lax.broadcasted_iota(jnp.int32, (2 * heads, half), 0)
    lane = lax.broadcasted_iota(jnp.int32, (2 * heads, half), 1)
    keep = ((lane ^ sub) & (heads - 1)) == 0

    def group_step(group, carry):
        run_max, run_sum, run_out = carry
        slot = lax.rem(group, KV_SLOTS)
        whole = pl.ds(0, GROUP * span_rows)

        @pl.when(group + KV_SLOTS - 1 < groups)
        def _():
            kv_start(group + KV_SLOTS - 1)
        pltpu.make_async_copy(kc_ref.at[0, whole], k_buf.at[slot], k_sem.at[slot]).wait()
        pltpu.make_async_copy(vc_ref.at[0, whole], v_buf.at[slot], v_sem.at[slot]).wait()
        rows = [item_row[group * GROUP + member] for member in range(GROUP)]
        scores = []
        for member in range(GROUP):
            base = member * span_rows
            k_cat = jnp.concatenate([k_buf[slot, base:base + half, :], k_buf[slot, base + half:base + 2 * half, :]], axis=1)
            s = lax.dot_general(qb_scr[rows[member]], k_cat, (((1,), (1,)), ((), ())), preferred_element_type=jnp.float32)
            scores.append(jnp.where(keep, s, -1e30))
        tops = []
        for s in scores:
            folded = jnp.maximum(s[:heads], s[heads:])
            tops.append(jnp.max(folded, axis=-1, keepdims=True))
        weights_in = [jnp.exp2((s - jnp.concatenate([top, top], axis=0)) * rate) for s, top in zip(scores, tops)]
        outs = []
        sums = []
        for member in range(GROUP):
            base = member * span_rows
            e = weights_in[member]
            sums.append(jnp.sum(e[:heads] + e[heads:], axis=-1, keepdims=True))
            v_cat = jnp.concatenate([v_buf[slot, base:base + half, :], v_buf[slot, base + half:base + 2 * half, :]], axis=1)
            both = jnp.dot(e.astype(jnp.bfloat16), v_cat, preferred_element_type=jnp.float32)
            outs.append(both[:heads, :head_dim] + both[heads:, head_dim:])
        for member in range(GROUP):
            row = rows[member]
            first = item_pos[group * GROUP + member] == 0
            run_max = jnp.where(first, s_scr[row], run_max)
            run_sum = jnp.where(first, 1.0, run_sum)
            run_out = jnp.where(first, v_scr[row], run_out)
            top = jnp.broadcast_to(tops[member], run_max.shape)
            new_max = jnp.maximum(run_max, top)
            keep_old = jnp.exp2((run_max - new_max) * rate)
            take_new = jnp.exp2((top - new_max) * rate)
            run_sum = run_sum * keep_old + take_new * sums[member]
            run_out = run_out * keep_old + take_new * outs[member]
            run_max = new_max
            o_scr[row] = run_out / run_sum
        return run_max, run_sum, run_out
    blank = jnp.zeros((heads, head_dim), jnp.float32)
    lax.fori_loop(0, groups, group_step, (blank, blank, blank))
    for head in range(heads):
        o_ref[:, head * head_dim:(head + 1) * head_dim] = o_scr[0:batch, head, :].astype(jnp.bfloat16)


def self_block(x, k_cache, v_cache, seq_lens, gain, bias, w_q, w_k, w_v):
    batch, width = x.shape
    ctx, heads, head_dim = k_cache.shape[1:]
    k_flat = k_cache.reshape(batch, ctx * heads, head_dim)
    v_flat = v_cache.reshape(batch, ctx * heads, head_dim)
    vmem = pl.BlockSpec(memory_space=pltpu.VMEM)
    hbm = pl.BlockSpec(memory_space=pl.ANY)
    flat = jax.ShapeDtypeStruct((batch, heads * head_dim), jnp.bfloat16)
    new = jax.ShapeDtypeStruct((batch, heads, head_dim), jnp.bfloat16)
    per_head = pltpu.VMEM((batch + 1, heads, head_dim), jnp.float32)
    kv_buf = pltpu.VMEM((KV_SLOTS, GROUP * SPAN * heads, head_dim), jnp.bfloat16)
    most_items = batch * ctx // SPAN + GROUP
    return pl.pallas_call(
        attn_kernel,
        out_shape=(flat, new, new),
        in_specs=[pl.BlockSpec(memory_space=pltpu.SMEM), vmem, vmem, vmem, hbm, hbm, hbm, hbm, hbm],
        out_specs=(vmem, vmem, vmem),
        scratch_shapes=[
            pltpu.VMEM((W_SLOTS, W_ROWS, heads * head_dim), jnp.bfloat16),
            kv_buf, kv_buf,
            pltpu.VMEM((width // W_ROWS, batch, W_ROWS), jnp.bfloat16),
            per_head,
            pltpu.VMEM((batch + 1, 2 * heads, 2 * head_dim), jnp.bfloat16),
            per_head, per_head, per_head, per_head,
            pltpu.VMEM((3, batch, heads * head_dim), jnp.float32),
            pltpu.SMEM((most_items,), jnp.int32),
            pltpu.SMEM((most_items,), jnp.int32),
            pltpu.SMEM((most_items,), jnp.int32),
            pltpu.SemaphoreType.DMA((W_SLOTS,)),
            pltpu.SemaphoreType.DMA((KV_SLOTS,)),
            pltpu.SemaphoreType.DMA((KV_SLOTS,)),
        ],
        compiler_params=pltpu.CompilerParams(vmem_limit_bytes=60 * 1024 * 1024),
        cost_estimate=pl.CostEstimate(flops=100_000_000_000, bytes_accessed=100_000_000, transcendentals=0),
        name='self_block',
    )(seq_lens, x, gain.reshape(1, width), bias.reshape(1, width), w_q, w_k, w_v, k_flat, v_flat)


RING = 15
LATE = 4
CUT = 256
QUAD = 512
SIDE = 1024


def mix_kernel(x_ref, o_ref, g2_ref, b2_ref, g3_ref, b3_ref, enc_ref, encm_ref, wkx_ref, wvx_ref, wo_ref, wq_ref, wk_ref, wv_ref, woc_ref, wup_ref, wdn_ref,
               out_ref,
               ring, e_buf, w_all, lhs, acc, h_scr, q_scr, q_send, q_recv, d_scr, p_scr, st_send, st_recv, o_mine, o_send, o_recv,
               ar_part, ar_half, ar_r1, ar_r2, ar_tot,
               ring_sem, e_sem, w_sem, x_sem, ex_send, ex_recv, y_send, y_recv, ar_send, ar_recv):
    batch, width = x_ref.shape
    head_dim = 128
    rate = head_dim ** -0.5 * LOG2_E
    dp = lax.axis_index('dp')
    tp = lax.axis_index('tp')
    core = lax.rem(tp, 2)
    mate = tp + 1 - 2 * core
    across = lax.rem(tp + 2, 4)
    other = 1 - dp
    to_mate, to_across, to_other = {'tp': mate}, {'tp': across}, {'dp': other}
    mesh_id = pl.DeviceIdType.MESH
    tokens = enc_ref.shape[1]
    spans = batch // 4

    barrier = pltpu.get_barrier_semaphore()
    for peer in (to_mate, to_across, to_other):
        pl.semaphore_signal(barrier, inc=1, device_id=peer, device_id_type=mesh_id)

    segments = ((wo_ref, 0, 4, False), (wq_ref, 4, 8, True), (woc_ref, 8, 12, False), (wup_ref, 12, 28, False), (wdn_ref, 28, 44 - LATE, False))

    def ring_copy(src, deep, row, slot, piece):
        if deep:
            view = src.at[pl.ds(row * SIDE + piece * CUT, CUT), :]
        else:
            view = src.at[pl.ds(row * CUT, CUT), pl.ds(piece * SIDE, SIDE)]
        return pltpu.make_async_copy(view, ring.at[slot, piece], ring_sem.at[slot, piece])

    def ring_start(index):
        for src, low, high, deep in segments:
            @pl.when((index >= low) & (index < high))
            def _():
                for piece in range(4):
                    ring_copy(src, deep, index - low, lax.rem(index, RING), piece).start()

    def slot_wait(slot):
        for piece in range(4):
            ring_copy(wo_ref, False, 0, slot, piece).wait()

    def ring_wait(index):
        slot = lax.rem(index, RING)
        slot_wait(slot)
        return slot

    def stream_wide(base, count, refill=True):
        acc[...] = jnp.zeros_like(acc)

        def step(chunk, carry):
            slot = ring_wait(base + chunk)
            for piece in range(4):
                acc[piece] += jnp.dot(lhs[chunk], ring[slot, piece], preferred_element_type=jnp.float32)
            if refill:
                ring_start(base + chunk + RING)
            return carry
        lax.fori_loop(0, count, step, 0)

    def late_start():
        for late in range(LATE):
            for piece in range(4):
                ring_copy(wdn_ref, False, 16 - LATE + late, RING + late, piece).start()

    def late_finish():
        def step(late, carry):
            slot_wait(RING + late)
            for piece in range(4):
                acc[piece] += jnp.dot(lhs[16 - LATE + late], ring[RING + late, piece], preferred_element_type=jnp.float32)
            return carry
        lax.fori_loop(0, LATE, step, 0)

    for index in range(4):
        for piece in range(4):
            ring_copy(wo_ref, False, index, index, piece).start()
    mine = pl.ds(pl.multiple_of(core * tokens, tokens), tokens)
    theirs_at = pl.ds(pl.multiple_of((1 - core) * tokens, tokens), tokens)
    e_local = pltpu.make_async_copy(enc_ref, e_buf.at[:, mine, :], e_sem.at[0])
    e_local.start()
    e_mate = pltpu.make_async_copy(encm_ref, e_buf.at[:, theirs_at, :], e_sem.at[1])
    e_mate.start()
    own_copies = []
    for kind, src in ((1, wv_ref), (0, wk_ref)):
        for quad in range(2):
            copy = pltpu.make_async_copy(src.at[:, pl.ds(quad * QUAD, QUAD)], w_all.at[kind, 0, :, pl.ds(quad * QUAD, QUAD)], w_sem.at[kind, quad])
            if kind == 1:
                copy.start()
            own_copies.append(copy)
    pl.semaphore_wait(barrier, 3)
    half_rows = wkx_ref.shape[0]
    crossed = (wkx_ref, wvx_ref)
    here = pl.ds(pl.multiple_of(dp * half_rows, half_rows), half_rows)

    def x_copy(kind):
        return pltpu.make_async_copy(crossed[kind], w_all.at[kind, 1, here, :], x_sem.at[kind])

    def y_copy(kind):
        return pltpu.make_async_remote_copy(src_ref=crossed[kind], dst_ref=w_all.at[kind, 1, here, :], send_sem=y_send.at[kind], recv_sem=y_recv.at[kind], device_id=to_other, device_id_type=mesh_id)

    for kind in range(2):
        y_copy(kind).start()

    def ar_copy(which, stage):
        if stage == 0:
            return pltpu.make_async_remote_copy(src_ref=ar_part.at[1 - core], dst_ref=ar_r1.at[which], send_sem=ar_send.at[which, 0], recv_sem=ar_recv.at[which, 0], device_id=to_mate, device_id_type=mesh_id)
        if stage == 1:
            return pltpu.make_async_remote_copy(src_ref=ar_half, dst_ref=ar_r2.at[which], send_sem=ar_send.at[which, 1], recv_sem=ar_recv.at[which, 1], device_id=to_across, device_id_type=mesh_id)
        return pltpu.make_async_remote_copy(src_ref=ar_tot.at[which, core], dst_ref=ar_tot.at[which, core], send_sem=ar_send.at[which, 2], recv_sem=ar_recv.at[which, 2], device_id=to_mate, device_id_type=mesh_id)

    def nothing():
        return None

    def reduce(which, first=nothing, second=nothing, third=nothing):
        for half in range(2):
            for piece in range(2):
                ar_part[half, :, piece * SIDE:(piece + 1) * SIDE] = acc[half * 2 + piece].astype(jnp.bfloat16)
        ar_copy(which, 0).start()
        first()
        ar_copy(which, 0).wait()
        ar_half[...] = (ar_part[core].astype(jnp.float32) + ar_r1[which].astype(jnp.float32)).astype(jnp.bfloat16)
        ar_copy(which, 1).start()
        second()
        ar_copy(which, 1).wait()
        ar_tot[which, core] = (ar_half[...].astype(jnp.float32) + ar_r2[which].astype(jnp.float32)).astype(jnp.bfloat16)
        ar_copy(which, 2).start()
        third()
        ar_copy(which, 2).wait()

    def total(which):
        return jnp.concatenate([ar_tot[which, 0].astype(jnp.float32), ar_tot[which, 1].astype(jnp.float32)], axis=1)

    def norm_into_lhs(values, gain_ref, bias_ref):
        row_mean = jnp.mean(values, axis=-1, keepdims=True)
        centred = values - row_mean
        row_var = jnp.mean(jnp.square(centred), axis=-1, keepdims=True)
        normed = (centred * lax.rsqrt(row_var + LN_EPS) * gain_ref[...] + bias_ref[...]).astype(jnp.bfloat16)
        for chunk in range(width // CUT):
            lhs[chunk] = normed[:, chunk * CUT:(chunk + 1) * CUT]

    def project_span(kind, side, quad, span):
        tile = e_buf[pl.ds(span * 4, 4)].reshape(4 * 2 * tokens, e_buf.shape[2])
        return jnp.dot(tile, w_all[kind, side, :, quad * QUAD:(quad + 1) * QUAD], preferred_element_type=jnp.float32).astype(jnp.bfloat16)

    row_id = lax.broadcasted_iota(jnp.int32, (16, QUAD), 0)
    col_tile = lax.broadcasted_iota(jnp.int32, (16, QUAD), 1) // head_dim
    head_match = row_id // 4 == col_tile
    seq_match = lax.rem(row_id, 4) == col_tile

    def keys_and_scores(side, quad):
        def step(span, carry):
            keys = project_span(0, side, quad, span)
            q4 = q_scr[side, quad, span]
            rows = jnp.where(head_match, jnp.concatenate([q4, q4, q4, q4], axis=0), 0.0).astype(jnp.bfloat16)
            s = lax.dot_general(rows, keys, (((1,), (1,)), ((), ())), preferred_element_type=jnp.float32)
            s = jnp.where(seq_match, s, 0.0)
            d_scr[side, quad, span] = s[:, 0:128] + s[:, 128:256] + s[:, 256:384] + s[:, 384:512]
            return carry
        lax.fori_loop(0, spans, step, 0, unroll=4)

    def own_values(quad, low, high):
        def step(span, carry):
            values = project_span(1, 0, quad, span)
            slot, piece = RING + quad * 2 + span // 4, span % 4
            ring[slot, piece, :, 0:QUAD] = values[0:CUT]
            ring[slot, piece, :, QUAD:SIDE] = values[CUT:2 * CUT]
            return carry
        lax.fori_loop(low, high, step, 0, unroll=2)

    def own_tile(quad, span):
        tile = ring[RING + quad * 2 + span // 4, span % 4]
        return jnp.concatenate([tile[:, 0:QUAD], tile[:, QUAD:SIDE]], axis=0)

    def apply_weights(side, quad, dest):
        def step(span, carry):
            values = own_tile(quad, span) if side == 0 else project_span(1, side, quad, span)
            p = p_scr[side, quad, span]
            rows = jnp.where(seq_match, jnp.concatenate([p, p, p, p], axis=1), 0.0).astype(jnp.bfloat16)
            wide = jnp.dot(rows, values, preferred_element_type=jnp.float32)
            wide = jnp.where(head_match, wide, 0.0)
            dest[quad, span] = wide[0:4] + wide[4:8] + wide[8:12] + wide[12:16]
            return carry
        lax.fori_loop(0, spans, step, 0, unroll=4)

    for chunk in range(4):
        lhs[chunk] = o_ref[:, chunk * CUT:(chunk + 1) * CUT]
    stream_wide(0, 4, refill=False)
    for index in range(4, 8):
        ring_start(jnp.int32(index))
    for copy in own_copies[2:]:
        copy.start()
    for kind in range(2):
        x_copy(kind).start()

    def open_values():
        e_local.wait()
        e_mate.wait()
        own_copies[0].wait()
        own_values(0, 0, 2)

    def more_values():
        own_copies[1].wait()
        own_values(1, 0, 2)
    reduce(0, open_values, lambda: own_values(0, 2, 8), more_values)
    h_one = x_ref[...].astype(jnp.float32) + total(0)
    h_scr[...] = h_one
    norm_into_lhs(h_one, g2_ref, b2_ref)

    def query_step(chunk, carry):
        slot = ring_wait(4 + chunk)
        for piece in range(4):
            acc[0] += jnp.dot(lhs[chunk * 4 + piece], ring[slot, piece], preferred_element_type=jnp.float32)
        return carry
    acc[0] = jnp.zeros_like(acc[0])
    lax.fori_loop(0, 4, query_step, 0)
    for index in range(8, 8 + RING):
        ring_start(jnp.int32(index))
    q_new = acc[0].astype(jnp.bfloat16)
    q_send[...] = q_new
    q_copy = pltpu.make_async_remote_copy(src_ref=q_send, dst_ref=q_recv, send_sem=ex_send.at[1], recv_sem=ex_recv.at[1], device_id=to_across, device_id_type=mesh_id)
    q_copy.start()

    def spread_query(side, q):
        wide = q.astype(jnp.float32)
        for quad in range(2):
            for span in range(spans):
                q_scr[side, quad, span] = wide[span * 4:span * 4 + 4, quad * QUAD:(quad + 1) * QUAD]
    spread_query(0, q_new)
    own_values(1, 2, 8)
    q_copy.wait()
    spread_query(1, q_recv[...])
    x_copy(0).wait()
    y_copy(0).wait_recv()
    keys_and_scores(1, 0)
    keys_and_scores(1, 1)

    lane = lax.broadcasted_iota(jnp.int32, (128, 128), 1)

    def block_stats(side, quad):
        s = d_scr[side, quad].reshape(128, 128)
        top = jnp.max(s, axis=-1, keepdims=True)
        part = jnp.sum(jnp.exp2((s - top) * rate), axis=-1, keepdims=True)
        return s, top, part

    def st_copy(side):
        return pltpu.make_async_remote_copy(src_ref=st_send.at[side], dst_ref=st_recv.at[side], send_sem=ex_send.at[2 * side], recv_sem=ex_recv.at[2 * side], device_id=to_across, device_id_type=mesh_id)

    def send_stats(side):
        for quad in range(2):
            s, top, part = block_stats(side, quad)
            packed = jnp.where(lane == 0, top, jnp.where(lane == 1, part, 0.0))
            st_send[side, quad] = packed.T[0:8, :]
        st_copy(side).start()

    def weights_of(side):
        for quad in range(2):
            s, top, part = block_stats(side, quad)
            theirs = jnp.concatenate([st_recv[1 - side, quad], jnp.zeros((120, 128), jnp.float32)], axis=0).T
            their_top, their_part = theirs[:, 0:1], theirs[:, 1:2]
            whole_top = jnp.maximum(top, their_top)
            whole = part * jnp.exp2((top - whole_top) * rate) + their_part * jnp.exp2((their_top - whole_top) * rate)
            p = jnp.exp2((s - whole_top) * rate) / whole
            p_scr[side, quad] = p.reshape(8, 16, 128)
    send_stats(1)
    own_copies[2].wait()
    own_copies[3].wait()
    keys_and_scores(0, 0)
    keys_and_scores(0, 1)
    send_stats(0)
    st_copy(1).wait()
    weights_of(0)
    apply_weights(0, 0, o_mine)
    apply_weights(0, 1, o_mine)
    late_start()
    st_copy(0).wait()
    weights_of(1)

    def o_copy(slot, quad):
        return pltpu.make_async_remote_copy(src_ref=o_send.at[quad], dst_ref=o_recv.at[quad], send_sem=ex_send.at[3 + slot], recv_sem=ex_recv.at[3 + slot], device_id=to_across, device_id_type=mesh_id)
    x_copy(1).wait()
    y_copy(1).wait_recv()
    apply_weights(1, 0, o_send)
    o_copy(0, 0).start()
    apply_weights(1, 1, o_send)
    o_copy(1, 1).start()
    o_copy(0, 0).wait()
    o_copy(1, 1).wait()
    for quad in range(2):
        whole = o_mine[quad] + o_recv[quad]
        whole = jnp.concatenate([whole[span] for span in range(spans)], axis=0).astype(jnp.bfloat16)
        for piece in range(2):
            lhs[quad * 2 + piece] = whole[:, piece * CUT:(piece + 1) * CUT]
    stream_wide(8, 4)
    reduce(1)
    h_two = h_scr[...] + total(1)
    h_scr[...] = h_two
    norm_into_lhs(h_two, g3_ref, b3_ref)
    stream_wide(12, 16)
    for piece in range(4):
        u = acc[piece]
        u = (0.5 * u * (1.0 + lax.erf(u * (0.5 ** 0.5)))).astype(jnp.bfloat16)
        for chunk in range(4):
            lhs[piece * 4 + chunk] = u[:, chunk * CUT:(chunk + 1) * CUT]
    stream_wide(28, 16 - LATE)
    late_finish()
    reduce(2)
    for kind in range(2):
        y_copy(kind).wait_send()
    out_ref[...] = (h_scr[...] + total(2)).astype(jnp.bfloat16)


def mix_block(x, self_out, nbr_enc, enc_mate, wk_cross, wv_cross, ln2_gain, ln2_bias, wq_c, wk_c, wv_c, w_o, wo_c, ln3_gain, ln3_bias, w_up, w_down):
    batch, width = x.shape
    _, tokens, enc = nbr_enc.shape
    vmem = pl.BlockSpec(memory_space=pltpu.VMEM)
    hbm = pl.BlockSpec(memory_space=pl.ANY)
    spans = batch // 4
    bf, f32 = jnp.bfloat16, jnp.float32
    dma = pltpu.SemaphoreType.DMA
    half = width // 2
    return pl.pallas_call(
        mix_kernel,
        out_shape=jax.ShapeDtypeStruct((batch, width), bf),
        in_specs=[vmem] * 6 + [hbm] * 11,
        out_specs=vmem,
        scratch_shapes=[
            pltpu.VMEM((RING + LATE, 4, CUT, SIDE), bf),
            pltpu.VMEM((batch, 2 * tokens, enc), bf),
            pltpu.VMEM((2, 2, enc, SIDE), bf),
            pltpu.VMEM((width // CUT, batch, CUT), bf),
            pltpu.VMEM((4, batch, SIDE), f32),
            pltpu.VMEM((batch, width), f32),
            pltpu.VMEM((2, 2, spans, 4, QUAD), f32),
            pltpu.VMEM((batch, SIDE), bf),
            pltpu.VMEM((batch, SIDE), bf),
            pltpu.VMEM((2, 2, spans, 16, 128), f32),
            pltpu.VMEM((2, 2, spans, 16, 128), f32),
            pltpu.VMEM((2, 2, 8, 128), f32),
            pltpu.VMEM((2, 2, 8, 128), f32),
            pltpu.VMEM((2, spans, 4, QUAD), f32),
            pltpu.VMEM((2, spans, 4, QUAD), f32),
            pltpu.VMEM((2, spans, 4, QUAD), f32),
            pltpu.VMEM((2, batch, half), bf),
            pltpu.VMEM((batch, half), bf),
            pltpu.VMEM((3, batch, half), bf),
            pltpu.VMEM((3, batch, half), bf),
            pltpu.VMEM((3, 2, batch, half), bf),
            dma((RING + LATE, 4)), dma((2,)), dma((2, 2)), dma((2,)), dma((5,)), dma((5,)), dma((2,)), dma((2,)), dma((3, 3)), dma((3, 3)),
        ],
        compiler_params=pltpu.CompilerParams(vmem_limit_bytes=67043328, collective_id=0, has_side_effects=True),
        name='mix_block',
    )(x, self_out, ln2_gain.reshape(1, width), ln2_bias.reshape(1, width), ln3_gain.reshape(1, width), ln3_bias.reshape(1, width), nbr_enc, enc_mate, wk_cross, wv_cross, w_o, wq_c, wk_c, wv_c, wo_c, w_up, w_down)


def local_step(x, k_cache, v_cache, seq_lens, nbr_enc, ln1_gain, ln1_bias, w_q, w_k, w_v, w_o, ln2_gain, ln2_bias, wq_c, wk_c, wv_c, wo_c, ln3_gain, ln3_bias, w_up, w_down):
    rows = wk_c.shape[0] // 2
    start = lax.axis_index('dp') * rows
    wk_cross, wv_cross = [lax.ppermute(lax.dynamic_slice_in_dim(w, start, rows, 0), 'tp', [(0, 2), (1, 3), (2, 0), (3, 1)]) for w in (wk_c, wv_c)]
    enc_mate = lax.ppermute(nbr_enc, 'tp', [(0, 1), (1, 0), (2, 3), (3, 2)])
    self_out, k_new, v_new = self_block(x, k_cache, v_cache, seq_lens, ln1_gain, ln1_bias, w_q, w_k, w_v)
    layer_out = mix_block(x, self_out, nbr_enc, enc_mate, wk_cross, wv_cross, ln2_gain, ln2_bias, wq_c, wk_c, wv_c, w_o, wo_c, ln3_gain, ln3_bias, w_up, w_down)
    return layer_out, k_new, v_new


def solution(mesh):
    row_spec = P('dp', None)
    cache_spec = P('dp', None, 'tp', None)
    head_spec = P('dp', 'tp', None)
    vec_spec = P(None)
    col_split = P(None, 'tp')
    row_split = P('tp', None)
    in_specs = (row_spec, cache_spec, cache_spec, P('dp'), P('dp', 'tp', None), vec_spec, vec_spec, col_split, col_split, col_split, row_split, vec_spec, vec_spec, col_split, col_split, col_split, row_split, vec_spec, vec_spec, col_split, row_split)
    out_specs = (row_spec, head_spec, head_spec)
    return jax.shard_map(local_step, mesh=mesh, in_specs=in_specs, out_specs=out_specs, check_vma=False)
```

```python
import jax
import jax.numpy as jnp
from jax import lax
from jax.experimental import pallas as pl
from jax.experimental.pallas import tpu as pltpu
from jax.sharding import PartitionSpec as P

LN_EPS = 1e-5
LOG2_E = 1.4426950408889634
W_SLOTS = 8
W_ROWS = 512
SPAN = 64
GROUP = 12
KV_SLOTS = 4


def attn_kernel(lens_ref, x_ref, g_ref, b_ref, wq_ref, wk_ref, wv_ref, kc_ref, vc_ref,
                o_ref, kn_ref, vn_ref,
                w_buf, k_buf, v_buf, a_scr, q_scr, qb_scr, k_scr, v_scr, s_scr, o_scr, acc_scr, item_row, item_src, item_pos, w_sem, k_sem, v_sem):
    batch, width = x_ref.shape
    heads = q_scr.shape[1]
    head_dim = q_scr.shape[2]
    rate = head_dim ** -0.5 * LOG2_E
    w_chunks = width // W_ROWS
    span_rows = SPAN * heads
    half = span_rows // 2
    weights = (wq_ref, wk_ref, wv_ref)

    def w_copy(index, src, row):
        slot = lax.rem(index, W_SLOTS)
        return pltpu.make_async_copy(src.at[pl.ds(row * W_ROWS, W_ROWS), :], w_buf.at[slot], w_sem.at[slot])

    for index in range(W_SLOTS):
        w_copy(jnp.int32(index), weights[index // w_chunks], index % w_chunks).start()

    def list_row(row, count):
        def list_span(span, count):
            item_row[count] = row
            item_src[count] = row
            item_pos[count] = span * span_rows
            return count + 1
        return lax.fori_loop(0, lax.div(lens_ref[row], SPAN), list_span, count)
    items = lax.fori_loop(0, batch, list_row, jnp.int32(0))
    groups = lax.div(items + (GROUP - 1), GROUP)
    for extra in range(GROUP):
        item_row[items + extra] = batch
        item_src[items + extra] = 0
        item_pos[items + extra] = 0

    def kv_start(group):
        slot = lax.rem(group, KV_SLOTS)
        for member in range(GROUP):
            item = group * GROUP + member
            rows = pl.ds(pl.multiple_of(item_pos[item], span_rows), span_rows)
            place = pl.ds(member * span_rows, span_rows)
            pltpu.make_async_copy(kc_ref.at[item_src[item], rows], k_buf.at[slot, place], k_sem.at[slot]).start()
            pltpu.make_async_copy(vc_ref.at[item_src[item], rows], v_buf.at[slot, place], v_sem.at[slot]).start()

    values = x_ref[...].astype(jnp.float32)
    row_mean = jnp.mean(values, axis=-1, keepdims=True)
    centred = values - row_mean
    row_var = jnp.mean(jnp.square(centred), axis=-1, keepdims=True)
    normed = (centred * lax.rsqrt(row_var + LN_EPS) * g_ref[...] + b_ref[...]).astype(jnp.bfloat16)
    for chunk in range(w_chunks):
        a_scr[chunk] = normed[:, chunk * W_ROWS:(chunk + 1) * W_ROWS]

    acc_scr[...] = jnp.zeros_like(acc_scr)

    def step(index, carry):
        which = lax.div(index, w_chunks)
        chunk = lax.rem(index, w_chunks)
        slot = lax.rem(index, W_SLOTS)
        w_copy(index, wq_ref, chunk).wait()
        acc_scr[which] += jnp.dot(a_scr[chunk], w_buf[slot], preferred_element_type=jnp.float32)
        later = index + W_SLOTS
        for source in range(1, 3):
            @pl.when(lax.div(later, w_chunks) == source)
            def _():
                w_copy(later, weights[source], lax.rem(later, w_chunks)).start()

        for ahead in range(KV_SLOTS - 1):
            @pl.when((index == 2 * w_chunks + ahead) & (ahead < groups))
            def _():
                kv_start(jnp.int32(ahead))
        return carry
    lax.fori_loop(0, 3 * w_chunks, step, 0)

    for which in range(3):
        out = acc_scr[which].astype(jnp.bfloat16)
        rounded = out.astype(jnp.float32)
        dest = (q_scr, k_scr, v_scr)[which]
        for head in range(heads):
            dest[0:batch, head, :] = rounded[:, head * head_dim:(head + 1) * head_dim]

    kn_ref[...] = k_scr[0:batch].astype(jnp.bfloat16)
    vn_ref[...] = v_scr[0:batch].astype(jnp.bfloat16)

    def prepare(row, carry):
        q = q_scr[row]
        zero = jnp.zeros_like(q)
        qb_scr[row] = jnp.concatenate([jnp.concatenate([q, zero], axis=1), jnp.concatenate([zero, q], axis=1)], axis=0).astype(jnp.bfloat16)
        s_scr[row] = jnp.broadcast_to(jnp.sum(q * k_scr[row], axis=-1, keepdims=True), q.shape)
        return carry
    lax.fori_loop(0, batch, prepare, 0, unroll=4)
    qb_scr[batch] = jnp.zeros(qb_scr.shape[1:], qb_scr.dtype)
    s_scr[batch] = jnp.zeros(s_scr.shape[1:], s_scr.dtype)
    v_scr[batch] = jnp.zeros(v_scr.shape[1:], v_scr.dtype)

    sub = lax.broadcasted_iota(jnp.int32, (2 * heads, half), 0)
    lane = lax.broadcasted_iota(jnp.int32, (2 * heads, half), 1)
    keep = ((lane ^ sub) & (heads - 1)) == 0

    def group_step(group, carry):
        run_max, run_sum, run_out = carry
        slot = lax.rem(group, KV_SLOTS)
        whole = pl.ds(0, GROUP * span_rows)

        @pl.when(group + KV_SLOTS - 1 < groups)
        def _():
            kv_start(group + KV_SLOTS - 1)
        pltpu.make_async_copy(kc_ref.at[0, whole], k_buf.at[slot], k_sem.at[slot]).wait()
        pltpu.make_async_copy(vc_ref.at[0, whole], v_buf.at[slot], v_sem.at[slot]).wait()
        rows = [item_row[group * GROUP + member] for member in range(GROUP)]
        scores = []
        for member in range(GROUP):
            base = member * span_rows
            k_cat = jnp.concatenate([k_buf[slot, base:base + half, :], k_buf[slot, base + half:base + 2 * half, :]], axis=1)
            s = lax.dot_general(qb_scr[rows[member]], k_cat, (((1,), (1,)), ((), ())), preferred_element_type=jnp.float32)
            scores.append(jnp.where(keep, s, -1e30))
        tops = []
        for s in scores:
            folded = jnp.maximum(s[:heads], s[heads:])
            tops.append(jnp.max(folded, axis=-1, keepdims=True))
        weights_in = [jnp.exp2((s - jnp.concatenate([top, top], axis=0)) * rate) for s, top in zip(scores, tops)]
        outs = []
        sums = []
        for member in range(GROUP):
            base = member * span_rows
            e = weights_in[member]
            sums.append(jnp.sum(e[:heads] + e[heads:], axis=-1, keepdims=True))
            v_cat = jnp.concatenate([v_buf[slot, base:base + half, :], v_buf[slot, base + half:base + 2 * half, :]], axis=1)
            both = jnp.dot(e.astype(jnp.bfloat16), v_cat, preferred_element_type=jnp.float32)
            outs.append(both[:heads, :head_dim] + both[heads:, head_dim:])
        for member in range(GROUP):
            row = rows[member]
            first = item_pos[group * GROUP + member] == 0
            run_max = jnp.where(first, s_scr[row], run_max)
            run_sum = jnp.where(first, 1.0, run_sum)
            run_out = jnp.where(first, v_scr[row], run_out)
            top = jnp.broadcast_to(tops[member], run_max.shape)
            new_max = jnp.maximum(run_max, top)
            keep_old = jnp.exp2((run_max - new_max) * rate)
            take_new = jnp.exp2((top - new_max) * rate)
            run_sum = run_sum * keep_old + take_new * sums[member]
            run_out = run_out * keep_old + take_new * outs[member]
            run_max = new_max
            o_scr[row] = run_out / run_sum
        return run_max, run_sum, run_out
    blank = jnp.zeros((heads, head_dim), jnp.float32)
    lax.fori_loop(0, groups, group_step, (blank, blank, blank))
    for head in range(heads):
        o_ref[:, head * head_dim:(head + 1) * head_dim] = o_scr[0:batch, head, :].astype(jnp.bfloat16)


def self_block(x, k_cache, v_cache, seq_lens, gain, bias, w_q, w_k, w_v):
    batch, width = x.shape
    ctx, heads, head_dim = k_cache.shape[1:]
    k_flat = k_cache.reshape(batch, ctx * heads, head_dim)
    v_flat = v_cache.reshape(batch, ctx * heads, head_dim)
    vmem = pl.BlockSpec(memory_space=pltpu.VMEM)
    hbm = pl.BlockSpec(memory_space=pl.ANY)
    flat = jax.ShapeDtypeStruct((batch, heads * head_dim), jnp.bfloat16)
    new = jax.ShapeDtypeStruct((batch, heads, head_dim), jnp.bfloat16)
    per_head = pltpu.VMEM((batch + 1, heads, head_dim), jnp.float32)
    kv_buf = pltpu.VMEM((KV_SLOTS, GROUP * SPAN * heads, head_dim), jnp.bfloat16)
    most_items = batch * ctx // SPAN + GROUP
    return pl.pallas_call(
        attn_kernel,
        out_shape=(flat, new, new),
        in_specs=[pl.BlockSpec(memory_space=pltpu.SMEM), vmem, vmem, vmem, hbm, hbm, hbm, hbm, hbm],
        out_specs=(vmem, vmem, vmem),
        scratch_shapes=[
            pltpu.VMEM((W_SLOTS, W_ROWS, heads * head_dim), jnp.bfloat16),
            kv_buf, kv_buf,
            pltpu.VMEM((width // W_ROWS, batch, W_ROWS), jnp.bfloat16),
            per_head,
            pltpu.VMEM((batch + 1, 2 * heads, 2 * head_dim), jnp.bfloat16),
            per_head, per_head, per_head, per_head,
            pltpu.VMEM((3, batch, heads * head_dim), jnp.float32),
            pltpu.SMEM((most_items,), jnp.int32),
            pltpu.SMEM((most_items,), jnp.int32),
            pltpu.SMEM((most_items,), jnp.int32),
            pltpu.SemaphoreType.DMA((W_SLOTS,)),
            pltpu.SemaphoreType.DMA((KV_SLOTS,)),
            pltpu.SemaphoreType.DMA((KV_SLOTS,)),
        ],
        compiler_params=pltpu.CompilerParams(vmem_limit_bytes=60 * 1024 * 1024),
        cost_estimate=pl.CostEstimate(flops=100_000_000_000, bytes_accessed=100_000_000, transcendentals=0),
        name='self_block',
    )(seq_lens, x, gain.reshape(1, width), bias.reshape(1, width), w_q, w_k, w_v, k_flat, v_flat)


RING = 15
LATE = 4
CUT = 256
QUAD = 512
SIDE = 1024


def mix_kernel(x_ref, o_ref, g2_ref, b2_ref, g3_ref, b3_ref, enc_ref, encm_ref, wkx_ref, wo_ref, wq_ref, wk_ref, wv_ref, woc_ref, wup_ref, wdn_ref,
               out_ref,
               ring, e_buf, w_all, lhs, acc, h_scr, q_scr, q_send, q_recv, d_scr, p_scr, st_send, st_recv, o_mine, o_send, o_recv,
               ar_part, ar_half, ar_r1, ar_r2, ar_tot,
               ring_sem, e_sem, w_sem, x_sem, ex_send, ex_recv, y_send, y_recv, vx_send, vx_recv, vy_send, vy_recv, ar_send, ar_recv):
    batch, width = x_ref.shape
    head_dim = 128
    rate = head_dim ** -0.5 * LOG2_E
    dp = lax.axis_index('dp')
    tp = lax.axis_index('tp')
    core = lax.rem(tp, 2)
    mate = tp + 1 - 2 * core
    across = lax.rem(tp + 2, 4)
    other = 1 - dp
    to_mate, to_across, to_other = {'tp': mate}, {'tp': across}, {'dp': other}
    mesh_id = pl.DeviceIdType.MESH
    tokens = enc_ref.shape[1]
    spans = batch // 4

    barrier = pltpu.get_barrier_semaphore()
    for peer in (to_mate, to_across, to_other):
        pl.semaphore_signal(barrier, inc=1, device_id=peer, device_id_type=mesh_id)

    segments = ((wo_ref, 0, 4, False), (wq_ref, 4, 8, True), (woc_ref, 8, 12, False), (wup_ref, 12, 28, False), (wdn_ref, 28, 44 - LATE, False))

    def ring_copy(src, deep, row, slot, piece):
        if deep:
            view = src.at[pl.ds(row * SIDE + piece * CUT, CUT), :]
        else:
            view = src.at[pl.ds(row * CUT, CUT), pl.ds(piece * SIDE, SIDE)]
        return pltpu.make_async_copy(view, ring.at[slot, piece], ring_sem.at[slot, piece])

    def ring_start(index):
        for src, low, high, deep in segments:
            @pl.when((index >= low) & (index < high))
            def _():
                for piece in range(4):
                    ring_copy(src, deep, index - low, lax.rem(index, RING), piece).start()

    def slot_wait(slot):
        for piece in range(4):
            ring_copy(wo_ref, False, 0, slot, piece).wait()

    def ring_wait(index):
        slot = lax.rem(index, RING)
        slot_wait(slot)
        return slot

    def stream_wide(base, count, refill=True):
        acc[...] = jnp.zeros_like(acc)

        def step(chunk, carry):
            slot = ring_wait(base + chunk)
            for piece in range(4):
                acc[piece] += jnp.dot(lhs[chunk], ring[slot, piece], preferred_element_type=jnp.float32)
            if refill:
                ring_start(base + chunk + RING)
            return carry
        lax.fori_loop(0, count, step, 0)

    def late_start():
        for late in range(LATE):
            for piece in range(4):
                ring_copy(wdn_ref, False, 16 - LATE + late, RING + late, piece).start()

    def late_finish():
        def step(late, carry):
            slot_wait(RING + late)
            for piece in range(4):
                acc[piece] += jnp.dot(lhs[16 - LATE + late], ring[RING + late, piece], preferred_element_type=jnp.float32)
            return carry
        lax.fori_loop(0, LATE, step, 0)

    for index in range(4):
        for piece in range(4):
            ring_copy(wo_ref, False, index, index, piece).start()
    mine = pl.ds(pl.multiple_of(core * tokens, tokens), tokens)
    theirs_at = pl.ds(pl.multiple_of((1 - core) * tokens, tokens), tokens)
    e_local = pltpu.make_async_copy(enc_ref, e_buf.at[:, mine, :], e_sem.at[0])
    e_local.start()
    e_mate = pltpu.make_async_copy(encm_ref, e_buf.at[:, theirs_at, :], e_sem.at[1])
    e_mate.start()
    own_copies = []
    for kind, src in ((1, wv_ref), (0, wk_ref)):
        for quad in range(2):
            copy = pltpu.make_async_copy(src.at[:, pl.ds(quad * QUAD, QUAD)], w_all.at[kind, 0, :, pl.ds(quad * QUAD, QUAD)], w_sem.at[kind, quad])
            if kind == 1:
                copy.start()
            own_copies.append(copy)
    pl.semaphore_wait(barrier, 3)
    half_rows = wkx_ref.shape[0]
    unit_rows = half_rows // 4
    here = pl.ds(pl.multiple_of(dp * half_rows, half_rows), half_rows)
    k_local = pltpu.make_async_copy(wkx_ref, w_all.at[0, 1, here, :], x_sem)
    k_across = pltpu.make_async_remote_copy(src_ref=wkx_ref, dst_ref=w_all.at[0, 1, here, :], send_sem=y_send, recv_sem=y_recv, device_id=to_other, device_id_type=mesh_id)

    def unit_place(unit):
        return pl.ds(pl.multiple_of(dp * half_rows + unit * unit_rows, unit_rows), unit_rows)

    def x_copy(unit):
        rows = unit_place(unit)
        return pltpu.make_async_remote_copy(src_ref=wv_ref.at[rows, :], dst_ref=w_all.at[1, 1, rows, :], send_sem=vx_send.at[unit], recv_sem=vx_recv.at[unit], device_id=to_across, device_id_type=mesh_id)

    def y_copy(unit):
        view = w_all.at[1, 1, unit_place(unit), :]
        return pltpu.make_async_remote_copy(src_ref=view, dst_ref=view, send_sem=vy_send.at[unit], recv_sem=vy_recv.at[unit], device_id=to_other, device_id_type=mesh_id)

    def relay(unit):
        x_copy(unit).wait_recv()
        y_copy(unit).start()

    k_across.start()
    x_copy(0).start()

    def ar_copy(which, stage):
        if stage == 0:
            return pltpu.make_async_remote_copy(src_ref=ar_part.at[1 - core], dst_ref=ar_r1.at[which], send_sem=ar_send.at[which, 0], recv_sem=ar_recv.at[which, 0], device_id=to_mate, device_id_type=mesh_id)
        if stage == 1:
            return pltpu.make_async_remote_copy(src_ref=ar_half, dst_ref=ar_r2.at[which], send_sem=ar_send.at[which, 1], recv_sem=ar_recv.at[which, 1], device_id=to_across, device_id_type=mesh_id)
        return pltpu.make_async_remote_copy(src_ref=ar_tot.at[which, core], dst_ref=ar_tot.at[which, core], send_sem=ar_send.at[which, 2], recv_sem=ar_recv.at[which, 2], device_id=to_mate, device_id_type=mesh_id)

    def nothing():
        return None

    def reduce(which, first=nothing, second=nothing, third=nothing):
        for half in range(2):
            for piece in range(2):
                ar_part[half, :, piece * SIDE:(piece + 1) * SIDE] = acc[half * 2 + piece].astype(jnp.bfloat16)
        ar_copy(which, 0).start()
        first()
        ar_copy(which, 0).wait()
        ar_half[...] = (ar_part[core].astype(jnp.float32) + ar_r1[which].astype(jnp.float32)).astype(jnp.bfloat16)
        ar_copy(which, 1).start()
        second()
        ar_copy(which, 1).wait()
        ar_tot[which, core] = (ar_half[...].astype(jnp.float32) + ar_r2[which].astype(jnp.float32)).astype(jnp.bfloat16)
        ar_copy(which, 2).start()
        third()
        ar_copy(which, 2).wait()

    def total(which):
        return jnp.concatenate([ar_tot[which, 0].astype(jnp.float32), ar_tot[which, 1].astype(jnp.float32)], axis=1)

    def norm_into_lhs(values, gain_ref, bias_ref):
        row_mean = jnp.mean(values, axis=-1, keepdims=True)
        centred = values - row_mean
        row_var = jnp.mean(jnp.square(centred), axis=-1, keepdims=True)
        normed = (centred * lax.rsqrt(row_var + LN_EPS) * gain_ref[...] + bias_ref[...]).astype(jnp.bfloat16)
        for chunk in range(width // CUT):
            lhs[chunk] = normed[:, chunk * CUT:(chunk + 1) * CUT]

    def project_span(kind, side, quad, span):
        tile = e_buf[pl.ds(span * 4, 4)].reshape(4 * 2 * tokens, e_buf.shape[2])
        return jnp.dot(tile, w_all[kind, side, :, quad * QUAD:(quad + 1) * QUAD], preferred_element_type=jnp.float32).astype(jnp.bfloat16)

    row_id = lax.broadcasted_iota(jnp.int32, (16, QUAD), 0)
    col_tile = lax.broadcasted_iota(jnp.int32, (16, QUAD), 1) // head_dim
    head_match = row_id // 4 == col_tile
    seq_match = lax.rem(row_id, 4) == col_tile

    def keys_and_scores(side, quad):
        def step(span, carry):
            keys = project_span(0, side, quad, span)
            q4 = q_scr[side, quad, span]
            rows = jnp.where(head_match, jnp.concatenate([q4, q4, q4, q4], axis=0), 0.0).astype(jnp.bfloat16)
            s = lax.dot_general(rows, keys, (((1,), (1,)), ((), ())), preferred_element_type=jnp.float32)
            s = jnp.where(seq_match, s, 0.0)
            d_scr[side, quad, span] = s[:, 0:128] + s[:, 128:256] + s[:, 256:384] + s[:, 384:512]
            return carry
        lax.fori_loop(0, spans, step, 0, unroll=4)

    def own_values(quad, low, high):
        def step(span, carry):
            values = project_span(1, 0, quad, span)
            slot, piece = RING + quad * 2 + span // 4, span % 4
            ring[slot, piece, :, 0:QUAD] = values[0:CUT]
            ring[slot, piece, :, QUAD:SIDE] = values[CUT:2 * CUT]
            return carry
        lax.fori_loop(low, high, step, 0, unroll=2)

    def own_tile(quad, span):
        tile = ring[RING + quad * 2 + span // 4, span % 4]
        return jnp.concatenate([tile[:, 0:QUAD], tile[:, QUAD:SIDE]], axis=0)

    def apply_weights(side, quad, dest):
        def step(span, carry):
            values = own_tile(quad, span) if side == 0 else project_span(1, side, quad, span)
            p = p_scr[side, quad, span]
            rows = jnp.where(seq_match, jnp.concatenate([p, p, p, p], axis=1), 0.0).astype(jnp.bfloat16)
            wide = jnp.dot(rows, values, preferred_element_type=jnp.float32)
            wide = jnp.where(head_match, wide, 0.0)
            dest[quad, span] = wide[0:4] + wide[4:8] + wide[8:12] + wide[12:16]
            return carry
        lax.fori_loop(0, spans, step, 0, unroll=4)

    for chunk in range(4):
        lhs[chunk] = o_ref[:, chunk * CUT:(chunk + 1) * CUT]
    stream_wide(0, 4, refill=False)
    for index in range(4, 8):
        ring_start(jnp.int32(index))
    for copy in own_copies[2:]:
        copy.start()
    k_local.start()

    def open_values():
        e_local.wait()
        e_mate.wait()
        own_copies[0].wait()
        own_values(0, 0, 2)

    def more_values():
        own_copies[1].wait()
        own_values(1, 0, 2)
    reduce(0, open_values, lambda: own_values(0, 2, 8), more_values)
    x_copy(1).start()
    relay(0)
    h_one = x_ref[...].astype(jnp.float32) + total(0)
    h_scr[...] = h_one
    norm_into_lhs(h_one, g2_ref, b2_ref)

    def query_step(chunk, carry):
        slot = ring_wait(4 + chunk)
        for piece in range(4):
            acc[0] += jnp.dot(lhs[chunk * 4 + piece], ring[slot, piece], preferred_element_type=jnp.float32)
        return carry
    acc[0] = jnp.zeros_like(acc[0])
    lax.fori_loop(0, 4, query_step, 0)
    for index in range(8, 8 + RING):
        ring_start(jnp.int32(index))
    q_new = acc[0].astype(jnp.bfloat16)
    q_send[...] = q_new
    q_copy = pltpu.make_async_remote_copy(src_ref=q_send, dst_ref=q_recv, send_sem=ex_send.at[1], recv_sem=ex_recv.at[1], device_id=to_across, device_id_type=mesh_id)
    q_copy.start()
    for unit in range(2, 4):
        x_copy(unit).start()

    def spread_query(side, q):
        wide = q.astype(jnp.float32)
        for quad in range(2):
            for span in range(spans):
                q_scr[side, quad, span] = wide[span * 4:span * 4 + 4, quad * QUAD:(quad + 1) * QUAD]
    spread_query(0, q_new)
    own_values(1, 2, 8)
    q_copy.wait()
    spread_query(1, q_recv[...])
    relay(1)
    k_local.wait()
    k_across.wait_recv()
    keys_and_scores(1, 0)
    relay(2)
    keys_and_scores(1, 1)
    relay(3)

    lane = lax.broadcasted_iota(jnp.int32, (128, 128), 1)

    def block_stats(side, quad):
        s = d_scr[side, quad].reshape(128, 128)
        top = jnp.max(s, axis=-1, keepdims=True)
        part = jnp.sum(jnp.exp2((s - top) * rate), axis=-1, keepdims=True)
        return s, top, part

    def st_copy(side):
        return pltpu.make_async_remote_copy(src_ref=st_send.at[side], dst_ref=st_recv.at[side], send_sem=ex_send.at[2 * side], recv_sem=ex_recv.at[2 * side], device_id=to_across, device_id_type=mesh_id)

    def send_stats(side):
        for quad in range(2):
            s, top, part = block_stats(side, quad)
            packed = jnp.where(lane == 0, top, jnp.where(lane == 1, part, 0.0))
            st_send[side, quad] = packed.T[0:8, :]
        st_copy(side).start()

    def weights_of(side):
        for quad in range(2):
            s, top, part = block_stats(side, quad)
            theirs = jnp.concatenate([st_recv[1 - side, quad], jnp.zeros((120, 128), jnp.float32)], axis=0).T
            their_top, their_part = theirs[:, 0:1], theirs[:, 1:2]
            whole_top = jnp.maximum(top, their_top)
            whole = part * jnp.exp2((top - whole_top) * rate) + their_part * jnp.exp2((their_top - whole_top) * rate)
            p = jnp.exp2((s - whole_top) * rate) / whole
            p_scr[side, quad] = p.reshape(8, 16, 128)
    send_stats(1)
    own_copies[2].wait()
    own_copies[3].wait()
    keys_and_scores(0, 0)
    keys_and_scores(0, 1)
    send_stats(0)
    st_copy(1).wait()
    weights_of(0)
    apply_weights(0, 0, o_mine)
    apply_weights(0, 1, o_mine)
    late_start()
    st_copy(0).wait()
    weights_of(1)

    def o_copy(slot, quad):
        return pltpu.make_async_remote_copy(src_ref=o_send.at[quad], dst_ref=o_recv.at[quad], send_sem=ex_send.at[3 + slot], recv_sem=ex_recv.at[3 + slot], device_id=to_across, device_id_type=mesh_id)
    for unit in range(4):
        y_copy(unit).wait_recv()
    apply_weights(1, 0, o_send)
    o_copy(0, 0).start()
    apply_weights(1, 1, o_send)
    o_copy(1, 1).start()
    o_copy(0, 0).wait()
    o_copy(1, 1).wait()
    for quad in range(2):
        whole = o_mine[quad] + o_recv[quad]
        whole = jnp.concatenate([whole[span] for span in range(spans)], axis=0).astype(jnp.bfloat16)
        for piece in range(2):
            lhs[quad * 2 + piece] = whole[:, piece * CUT:(piece + 1) * CUT]
    stream_wide(8, 4)
    reduce(1)
    h_two = h_scr[...] + total(1)
    h_scr[...] = h_two
    norm_into_lhs(h_two, g3_ref, b3_ref)
    stream_wide(12, 16)
    for piece in range(4):
        u = acc[piece]
        u = (0.5 * u * (1.0 + lax.erf(u * (0.5 ** 0.5)))).astype(jnp.bfloat16)
        for chunk in range(4):
            lhs[piece * 4 + chunk] = u[:, chunk * CUT:(chunk + 1) * CUT]
    stream_wide(28, 16 - LATE)
    late_finish()
    reduce(2)
    k_across.wait_send()
    for unit in range(4):
        x_copy(unit).wait_send()
        y_copy(unit).wait_send()
    out_ref[...] = (h_scr[...] + total(2)).astype(jnp.bfloat16)


def mix_block(x, self_out, nbr_enc, enc_mate, wk_cross, ln2_gain, ln2_bias, wq_c, wk_c, wv_c, w_o, wo_c, ln3_gain, ln3_bias, w_up, w_down):
    batch, width = x.shape
    _, tokens, enc = nbr_enc.shape
    vmem = pl.BlockSpec(memory_space=pltpu.VMEM)
    hbm = pl.BlockSpec(memory_space=pl.ANY)
    spans = batch // 4
    bf, f32 = jnp.bfloat16, jnp.float32
    dma = pltpu.SemaphoreType.DMA
    half = width // 2
    return pl.pallas_call(
        mix_kernel,
        out_shape=jax.ShapeDtypeStruct((batch, width), bf),
        in_specs=[vmem] * 6 + [hbm] * 10,
        out_specs=vmem,
        scratch_shapes=[
            pltpu.VMEM((RING + LATE, 4, CUT, SIDE), bf),
            pltpu.VMEM((batch, 2 * tokens, enc), bf),
            pltpu.VMEM((2, 2, enc, SIDE), bf),
            pltpu.VMEM((width // CUT, batch, CUT), bf),
            pltpu.VMEM((4, batch, SIDE), f32),
            pltpu.VMEM((batch, width), f32),
            pltpu.VMEM((2, 2, spans, 4, QUAD), f32),
            pltpu.VMEM((batch, SIDE), bf),
            pltpu.VMEM((batch, SIDE), bf),
            pltpu.VMEM((2, 2, spans, 16, 128), f32),
            pltpu.VMEM((2, 2, spans, 16, 128), f32),
            pltpu.VMEM((2, 2, 8, 128), f32),
            pltpu.VMEM((2, 2, 8, 128), f32),
            pltpu.VMEM((2, spans, 4, QUAD), f32),
            pltpu.VMEM((2, spans, 4, QUAD), f32),
            pltpu.VMEM((2, spans, 4, QUAD), f32),
            pltpu.VMEM((2, batch, half), bf),
            pltpu.VMEM((batch, half), bf),
            pltpu.VMEM((3, batch, half), bf),
            pltpu.VMEM((3, batch, half), bf),
            pltpu.VMEM((3, 2, batch, half), bf),
            dma((RING + LATE, 4)), dma((2,)), dma((2, 2)), dma, dma((5,)), dma((5,)), dma, dma, dma((4,)), dma((4,)), dma((4,)), dma((4,)), dma((3, 3)), dma((3, 3)),
        ],
        compiler_params=pltpu.CompilerParams(vmem_limit_bytes=67043328, collective_id=0, has_side_effects=True),
        name='mix_block',
    )(x, self_out, ln2_gain.reshape(1, width), ln2_bias.reshape(1, width), ln3_gain.reshape(1, width), ln3_bias.reshape(1, width), nbr_enc, enc_mate, wk_cross, w_o, wq_c, wk_c, wv_c, wo_c, w_up, w_down)


def local_step(x, k_cache, v_cache, seq_lens, nbr_enc, ln1_gain, ln1_bias, w_q, w_k, w_v, w_o, ln2_gain, ln2_bias, wq_c, wk_c, wv_c, wo_c, ln3_gain, ln3_bias, w_up, w_down):
    rows = wk_c.shape[0] // 2
    start = lax.axis_index('dp') * rows
    wk_cross = lax.ppermute(lax.dynamic_slice_in_dim(wk_c, start, rows, 0), 'tp', [(0, 2), (1, 3), (2, 0), (3, 1)])
    enc_mate = lax.ppermute(nbr_enc, 'tp', [(0, 1), (1, 0), (2, 3), (3, 2)])
    self_out, k_new, v_new = self_block(x, k_cache, v_cache, seq_lens, ln1_gain, ln1_bias, w_q, w_k, w_v)
    layer_out = mix_block(x, self_out, nbr_enc, enc_mate, wk_cross, ln2_gain, ln2_bias, wq_c, wk_c, wv_c, w_o, wo_c, ln3_gain, ln3_bias, w_up, w_down)
    return layer_out, k_new, v_new


def solution(mesh):
    row_spec = P('dp', None)
    cache_spec = P('dp', None, 'tp', None)
    head_spec = P('dp', 'tp', None)
    vec_spec = P(None)
    col_split = P(None, 'tp')
    row_split = P('tp', None)
    in_specs = (row_spec, cache_spec, cache_spec, P('dp'), P('dp', 'tp', None), vec_spec, vec_spec, col_split, col_split, col_split, row_split, vec_spec, vec_spec, col_split, col_split, col_split, row_split, vec_spec, vec_spec, col_split, row_split)
    out_specs = (row_spec, head_spec, head_spec)
    return jax.shard_map(local_step, mesh=mesh, in_specs=in_specs, out_specs=out_specs, check_vma=False)
```
